32 devices in a mesh: slab: 8 (over z, y), shot: 4 (over x, core).
Axes of the slice: x: 2, y: 2, z: 4, core: 2. Of those that a mesh axis runs over, the one named last changes fastest.
Arguments:
- velocity: float32 [8, 512, 512], P('slab'), may hold values from 1.5 to 4.5
- initial_field: float32 [4, 8, 256, 256], P('shot', 'slab'), may hold values from -6 to 6
- anchor_x: int32 [4], P('shot'), may hold values from 0 to 256
- anchor_y: int32 [4], P('shot'), may hold values from 0 to 256
- source_cell: int32 [4], P('shot'), may hold values from 0 to 65535
- receivers: int32 [4, 256], P('shot'), may hold values from 0 to 65535
Outputs:
- traces: float32 [4, 4, 256], P('shot')
- image: float32 [8, 512, 512], P('slab', 'shot')
The draws below stay inside these ranges and needn't reach their ends.
Inputs may be any that keep to these rules, and one draw needn't show every extreme that they name: `anchor_x`: shot i's window lies inside the model. `anchor_y`: shot i's window lies inside the model.
All inputs are finite; a program needn't handle non-finite values.
Results may differ from the reference program's by a relative error of at most 0.0003.
Values sent between devices are 32-bit elements; how exact they have to be, the bound alone decides.
No kernel may reach another device: no remote copies, remote signals or barrier semaphores. Data moves between devices by JAX's collectives and lax.ppermute only.
A program may use at most 64 MiB of HBM per device.

```python
import math
import jax
import jax.numpy as jnp
from jax import lax

MX = 512
MY = 512
AWX = 256
AWY = 256
NREC = 256
STEPS = 4
NZ = 8
SHOTS = 4


def set_ends(result, own_key, low, top_value):
    dims = result.shape
    index_at = [jax.random.randint(jax.random.fold_in(own_key, axis), (), 0, dims[axis]) for axis in range(len(dims))]
    result = result.at[tuple(index_at)].set(low)
    longest = dims.index(max(dims))
    index_at[longest] = (index_at[longest] + 1) % dims[longest]
    return result.at[tuple(index_at)].set(top_value)


def steps_of(stream_key, dims, pieces, least, high):
    loudness, own = 1.0, jax.random.fold_in(stream_key, 6)
    for position, parts in pieces:
        steps = jnp.exp(jax.random.uniform(jax.random.fold_in(own, position), (parts,), jnp.float32, least / len(pieces), high / len(pieces)))
        loudness = loudness * jnp.repeat(steps, dims[position] // parts).reshape([-1 if axis == position else 1 for axis in range(len(dims))])
    return loudness


def noise(key, extent, scale, most, shards=(), kind=jnp.bfloat16):
    values = jax.random.normal(key, extent, jnp.float32) * scale
    if len(shards) > 0:
        values = steps_of(key, extent, shards, -0.22, 0.18) * values
    return jnp.clip(values, min=-most, max=most).astype(kind)


def setup_inputs(seed: int = 0) -> dict:
    key_of = jax.random.split(jax.random.key(seed), 7)
    return {
        "velocity": jnp.clip(1.5 + 3.0 * jax.random.uniform(key_of[0], (NZ, MX, MY), jnp.float32) ** steps_of(key_of[0], (NZ, MX, MY), ((0, 8),), -0.2, 0.2), 1.5, 4.5),
        "initial_field": noise(key_of[1], (SHOTS, NZ, AWX, AWY), 1.0, 6.0, ((0, 4), (1, 8)), jnp.float32),
        "anchor_x": set_ends(jax.random.randint(key_of[2], (SHOTS,), 0, MX - AWX + 1), jax.random.fold_in(key_of[2], 1), 0, MX - AWX).astype(jnp.int32),
        "anchor_y": set_ends(jax.random.randint(key_of[3], (SHOTS,), 0, MY - AWY + 1), jax.random.fold_in(key_of[3], 1), 0, MY - AWY).astype(jnp.int32),
        "source_cell": set_ends(jax.random.randint(key_of[4], (SHOTS,), 0, AWX * AWY), jax.random.fold_in(key_of[4], 1), 0, (AWX * AWY) - 1).astype(jnp.int32),
        "receivers": set_ends(jax.random.randint(key_of[5], (SHOTS, NREC), 0, AWX * AWY), jax.random.fold_in(key_of[5], 1), 0, (AWX * AWY) - 1).astype(jnp.int32),
    }


COURANT = 0.125
AMPLITUDE = 4.0


def wavelet(instant):
    shifted = 0.8 * (instant - 1.5)
    return (1.0 - 2.0 * shifted * shifted) * math.exp(-shifted * shifted)


def propagate(window, pressure, source, receiver_row):
    coefficient = jnp.square(COURANT * window)
    layers, rows_x, cols_y = window.shape
    flat_index = jnp.arange(rows_x * cols_y, dtype=jnp.int32).reshape(rows_x, cols_y)
    source_plane = (flat_index == source).astype(window.dtype)
    previous = pressure
    current = pressure
    energy = jnp.zeros(window.shape, window.dtype)
    samples = []
    for instant in range(STEPS):
        padded = jnp.pad(current, 1)
        laplacian = padded[2:, 1:-1, 1:-1] + padded[:-2, 1:-1, 1:-1]
        laplacian = laplacian + padded[1:-1, 2:, 1:-1] + padded[1:-1, :-2, 1:-1]
        laplacian = laplacian + padded[1:-1, 1:-1, 2:] + padded[1:-1, 1:-1, :-2]
        laplacian = laplacian - 6.0 * current
        advanced = 2.0 * current - previous + coefficient * laplacian
        advanced = advanced.at[1].add(coefficient[1] * source_plane * (AMPLITUDE * wavelet(instant)))
        energy = energy + advanced * advanced
        samples.append(jnp.take(advanced[0].reshape(-1), receiver_row))
        previous, current = current, advanced
    return energy / STEPS, jnp.stack(samples)


def reference(velocity, initial_field, anchor_x, anchor_y, source_cell, receivers):
    def one_shot(stacked, inputs):
        pressure, start_x, start_y, source, receiver_row = inputs
        corner = (jnp.int32(0), start_x.astype(jnp.int32), start_y.astype(jnp.int32))
        window = lax.dynamic_slice(velocity, corner, (NZ, AWX, AWY))
        energy, samples = propagate(window, pressure, source, receiver_row)
        placed = lax.dynamic_slice(stacked, corner, (NZ, AWX, AWY)) + energy
        return lax.dynamic_update_slice(stacked, placed, corner), samples

    start = jnp.zeros(velocity.shape, velocity.dtype)
    stacked, traces = lax.scan(one_shot, start, (initial_field, anchor_x, anchor_y, source_cell, receivers))
    return traces, stacked
```

```python
import math

import jax
import jax.numpy as jnp
from jax import lax
from jax.experimental import pallas as pl
from jax.experimental.pallas import tpu as pltpu
from jax.sharding import PartitionSpec as P

STEPS = 4


COURANT = 0.125
AMPLITUDE = 4.0

SUBLANES = 8
LANES = 128


def wavelet(instant):
    shifted = 0.8 * (instant - 1.5)
    return (1.0 - 2.0 * shifted * shifted) * math.exp(-shifted * shifted)


def with_halo(cells, sides, width):
    for axis, dim in sides:
        count = lax.axis_size(axis)
        ends = count - 1
        head = lax.slice_in_dim(cells, 0, width, axis=dim)
        tail = lax.slice_in_dim(cells, cells.shape[dim] - width, cells.shape[dim], axis=dim)
        cells = jnp.concatenate(
            [
                lax.ppermute(tail, axis, [(i, (i + 1) % count) for i in range(ends)]),
                cells,
                lax.ppermute(head, axis, [((i + 1) % count, i) for i in range(ends)]),
            ],
            axis=dim,
        )
    return cells


def propagate(speed, field, extend, source, depth_start):
    coefficient = jnp.square(COURANT * speed)
    column_count = speed.shape[3]
    depth_place = lax.broadcasted_iota(jnp.int32, speed.shape, 1) + depth_start
    row_place = lax.broadcasted_iota(jnp.int32, speed.shape, 2)
    column_place = lax.broadcasted_iota(jnp.int32, speed.shape, 3)
    source_row = (source // column_count)[:, None, None, None]
    source_column = (source % column_count)[:, None, None, None]
    struck = (depth_place == 1) & (row_place == source_row) & (column_place == source_column)
    source_term = jnp.where(struck, coefficient, jnp.float32(0.0))
    previous = field
    current = field
    energy = jnp.zeros(speed.shape, jnp.float32)
    surfaces = []
    for instant in range(STEPS):
        padded = extend(current)
        laplacian = padded[:, 2:, 1:-1, 1:-1] + padded[:, :-2, 1:-1, 1:-1]
        laplacian = laplacian + padded[:, 1:-1, 2:, 1:-1] + padded[:, 1:-1, :-2, 1:-1]
        laplacian = laplacian + padded[:, 1:-1, 1:-1, 2:] + padded[:, 1:-1, 1:-1, :-2]
        laplacian = laplacian - 6.0 * current
        advanced = 2.0 * current - previous + coefficient * laplacian
        advanced = advanced + source_term * (AMPLITUDE * wavelet(instant))
        energy = energy + advanced * advanced
        surfaces.append(advanced[:, 0])
        previous, current = (current, advanced)
    return (energy / STEPS, jnp.stack(surfaces, axis=1))


def by_depth(velocity, initial_field, anchor_x, anchor_y, source_cell, receivers):
    slab_index = lax.axis_index("slab")
    layers, width_x, width_y = velocity.shape
    shot_count = initial_field.shape[0]
    window_rows = initial_field.shape[2]
    window_cols = initial_field.shape[3]

    def cut_window(start_x, start_y):
        return lax.dynamic_slice(
            velocity, (jnp.int32(0), start_x, start_y), (layers, window_rows, window_cols)
        )

    windows = jax.vmap(cut_window)(anchor_x, anchor_y)
    depth_start = slab_index * layers

    def extend_depth(current):
        rimmed = with_halo(current, (("slab", 1),), 1)
        return jnp.pad(rimmed, ((0, 0), (0, 0), (1, 1), (1, 1)))

    energy_here, surface = propagate(windows, initial_field, extend_depth, source_cell, depth_start)
    local_rows = surface.shape[2]
    receiver_row = receivers // window_cols
    receiver_column = receivers % window_cols
    holds = (receiver_row >= 0) & (receiver_row < local_rows) & (depth_start == 0)
    flat_local = jnp.clip(receiver_row, 0, local_rows - 1) * window_cols + receiver_column
    record_count = receivers.shape[1]
    picked = jnp.take_along_axis(
        surface.reshape(shot_count, STEPS, -1),
        jnp.broadcast_to(flat_local[:, None, :], (shot_count, STEPS, record_count)),
        axis=2,
    )
    picked = jnp.where(holds[:, None, :], picked, jnp.float32(0.0))
    traces = lax.psum(picked, "slab")
    partial_image = jnp.zeros((layers, width_x, width_y), jnp.float32)
    corner = (jnp.int32(0), anchor_x[0], anchor_y[0])
    partial_image = lax.dynamic_update_slice(partial_image, energy_here[0], corner)
    summed = lax.psum_scatter(partial_image, "shot", scatter_dimension=1, tiled=True)
    return (traces, summed)


def strip_pack(window_rows, window_cols, slabs, strip):
    tall = strip + 2 * STEPS

    def body(anchor_x, anchor_y, velocity, field, *rest):
        blocks, (planes,) = rest[:slabs], rest[slabs:]
        mine = lax.axis_index("slab")
        top, left = anchor_x[0], anchor_y[0]
        rolled = pltpu.roll(field[0, 0], left % window_cols, axis=1)
        rolled = pltpu.roll(rolled, (top + STEPS) % window_rows, axis=0)
        planes[0, :window_rows] = rolled
        planes[0, window_rows:] = rolled[: 2 * STEPS]
        rows = lax.broadcasted_iota(jnp.int32, (window_rows, window_cols), 0)
        columns = lax.broadcasted_iota(jnp.int32, (window_rows, window_cols), 1)
        near = jnp.where(columns >= left, velocity[0, :window_rows, :window_cols], velocity[0, :window_rows, window_cols:])
        far = jnp.where(columns >= left, velocity[0, window_rows:, :window_cols], velocity[0, window_rows:, window_cols:])
        speed = COURANT * jnp.where(rows >= top, near, far)
        coefficient = pltpu.roll(speed * speed, STEPS, axis=0)
        planes[1, :window_rows] = coefficient
        planes[1, window_rows:] = coefficient[: 2 * STEPS]
        for k in range(slabs):
            start = pl.multiple_of((mine ^ k) * strip, SUBLANES)
            blocks[k][:tall] = planes[0, pl.ds(start, tall), :]
            blocks[k][tall:] = planes[1, pl.ds(start, tall), :]

    smem = pl.BlockSpec(memory_space=pltpu.SMEM)
    vmem = pl.BlockSpec(memory_space=pltpu.VMEM)
    return pl.pallas_call(
        body,
        out_shape=[jax.ShapeDtypeStruct((2 * tall, window_cols), jnp.float32)] * slabs,
        in_specs=[smem, smem, vmem, vmem],
        out_specs=[vmem] * slabs,
        scratch_shapes=[pltpu.VMEM((2, window_rows + 2 * STEPS, window_cols), jnp.float32)],
        name="strip_pack",
    )


def strip_steps(window_rows, window_cols, slabs, strip, records):
    tall = strip + 2 * STEPS

    def body(anchor_x, anchor_y, source, receivers, *rest):
        blocks, outs, (fields, speeds, energy, surface) = rest[:slabs], rest[slabs : 2 * slabs], rest[2 * slabs :]
        mine = lax.axis_index("slab")
        top, left = anchor_x[0], anchor_y[0]
        for k in range(slabs):
            fields[0, mine ^ k] = blocks[k][:tall]
            speeds[mine ^ k] = blocks[k][tall:]
        rows = lax.broadcasted_iota(jnp.int32, (tall, window_cols), 0)
        columns = lax.broadcasted_iota(jnp.int32, (tall, window_cols), 1)

        def local_row(row):
            return (row + top - mine * strip + STEPS + window_rows) % window_rows

        def local_column(column):
            return (column + left) % window_cols

        inside_up = rows != local_row(0)
        inside_down = rows != local_row(window_rows - 1)
        inside_left = columns != local_column(0)
        inside_right = columns != local_column(window_cols - 1)
        struck = (rows == local_row(source[0] // window_cols)) & (columns == local_column(source[0] % window_cols))
        source_term = jnp.where(struck, speeds[1], 0.0)
        for instant in range(STEPS):
            now, then = instant % 2, (instant + 1) % 2
            for level in range(slabs):
                current = fields[now, level]
                previous = fields[then if instant else now, level]
                laplacian = jnp.where(inside_up, pltpu.roll(current, 1, axis=0), 0.0)
                laplacian = laplacian + jnp.where(inside_down, pltpu.roll(current, tall - 1, axis=0), 0.0)
                laplacian = laplacian + jnp.where(inside_left, pltpu.roll(current, 1, axis=1), 0.0)
                laplacian = laplacian + jnp.where(inside_right, pltpu.roll(current, window_cols - 1, axis=1), 0.0)
                if level > 0:
                    laplacian = laplacian + fields[now, level - 1]
                if level < slabs - 1:
                    laplacian = laplacian + fields[now, level + 1]
                laplacian = laplacian - 6.0 * current
                advanced = 2.0 * current - previous + speeds[level] * laplacian
                if level == 1:
                    advanced = advanced + source_term * (AMPLITUDE * wavelet(instant))
                if level == 0:
                    surface[instant * tall : (instant + 1) * tall] = advanced
                if instant < STEPS - 1:
                    fields[then, level] = advanced
                square = advanced * advanced
                energy[level] = square if instant == 0 else energy[level] + square
        row = receivers[...] // window_cols
        column = (receivers[...] % window_cols + left) % window_cols
        row = (row + top) % window_rows - mine * strip + STEPS
        row = jnp.where((row >= STEPS) & (row < STEPS + strip), row, -1)
        cells = lax.broadcasted_iota(jnp.int32, (window_cols, records), 0)
        chosen = jnp.where(cells == column, 1.0, 0.0)
        picked = jnp.dot(surface[...], chosen, precision=lax.Precision.HIGHEST, preferred_element_type=jnp.float32)
        places = lax.broadcasted_iota(jnp.int32, (tall, records), 0)
        heard = [
            jnp.sum(jnp.where(places == row, picked[i * tall : (i + 1) * tall], 0.0), axis=0, keepdims=True)
            for i in range(STEPS)
        ]
        pieces = window_cols // LANES
        for k in range(slabs):
            for i in range(pieces):
                outs[k][i * strip : (i + 1) * strip] = (
                    energy[mine ^ k, STEPS : STEPS + strip, i * LANES : (i + 1) * LANES] / STEPS
                )
            for i in range(records // LANES):
                for n in range(STEPS):
                    at = pieces * strip + i * STEPS + n
                    outs[k][at : at + 1] = heard[n][:, i * LANES : (i + 1) * LANES]

    smem = pl.BlockSpec(memory_space=pltpu.SMEM)
    vmem = pl.BlockSpec(memory_space=pltpu.VMEM)
    deep = window_cols // LANES * strip + records // LANES * STEPS
    return pl.pallas_call(
        body,
        out_shape=[jax.ShapeDtypeStruct((deep, LANES), jnp.float32)] * slabs,
        in_specs=[smem, smem, smem, vmem] + [vmem] * slabs,
        out_specs=[vmem] * slabs,
        scratch_shapes=[
            pltpu.VMEM((2, slabs, tall, window_cols), jnp.float32),
            pltpu.VMEM((slabs, tall, window_cols), jnp.float32),
            pltpu.VMEM((slabs, tall, window_cols), jnp.float32),
            pltpu.VMEM((STEPS * tall, window_cols), jnp.float32),
        ],
        name="strip_steps",
    )


def strip_gather(window_rows, window_cols, slabs, shots, strip, records):
    pieces = window_cols // LANES
    parts = slabs * strip // (window_rows // 2)
    half = window_rows // parts
    per_half = half // strip
    size = pieces * half + SUBLANES

    def body(anchor_x, anchor_y, *rest):
        blocks, (traces, same, other), (energy,) = rest[:slabs], rest[slabs : slabs + 3], rest[slabs + 3 :]
        mine = lax.axis_index("slab")
        core = lax.axis_index("shot") % 2
        total = blocks[0][pieces * strip :]
        for k in range(1, slabs):
            total = total + blocks[k][pieces * strip :]
        for i in range(records // LANES):
            traces[0, :, i * LANES : (i + 1) * LANES] = total[i * STEPS : (i + 1) * STEPS]
        for k in range(slabs):
            place = mine ^ k
            side = jnp.where(place // per_half == core, 0, 1)
            for i in range(pieces):
                start = pl.multiple_of(i * half + place % per_half * strip, SUBLANES)
                energy[side, pl.ds(start, strip), :] = blocks[k][i * strip : (i + 1) * strip]
        where_x = anchor_x[0].astype(jnp.float32)
        where_y = anchor_y[0].astype(jnp.float32)
        tags = lax.broadcasted_iota(jnp.int32, (SUBLANES, LANES), 0)
        tag = jnp.where(tags == 0, where_x, where_y)
        for side, out in enumerate((same, other)):
            out[: pieces * half] = energy[side]
            out[pieces * half :] = tag

    smem = pl.BlockSpec(memory_space=pltpu.SMEM)
    vmem = pl.BlockSpec(memory_space=pltpu.VMEM)
    return pl.pallas_call(
        body,
        out_shape=[
            jax.ShapeDtypeStruct((1, STEPS, records), jnp.float32),
            jax.ShapeDtypeStruct((size, LANES), jnp.float32),
            jax.ShapeDtypeStruct((size, LANES), jnp.float32),
        ],
        in_specs=[smem, smem] + [vmem] * slabs,
        out_specs=[vmem] * 3,
        scratch_shapes=[pltpu.VMEM((2, pieces * half, LANES), jnp.float32)],
        name="strip_gather",
    )


def strip_image(window_rows, window_cols, width_y, rows_here, count):
    pieces = window_cols // LANES

    def body(*rest):
        blocks, image = rest[:count], rest[count]
        first = lax.axis_index("shot") * rows_here
        rows = lax.broadcasted_iota(jnp.int32, (rows_here, LANES), 0) + first
        columns = lax.broadcasted_iota(jnp.int32, (rows_here, LANES), 1)
        tags = [block[pieces * rows_here :].astype(jnp.int32) for block in blocks]
        for i in range(width_y // LANES):
            total = jnp.zeros((rows_here, LANES), jnp.float32)
            for block, tag in zip(blocks, tags):
                down = rows - tag[0:1]
                along = columns + i * LANES - tag[1:2]
                inside = (down >= 0) & (down < window_rows) & (along >= 0) & (along < window_cols)
                piece = i % pieces
                total = total + jnp.where(inside, block[piece * rows_here : (piece + 1) * rows_here], 0.0)
            image[0, :, i * LANES : (i + 1) * LANES] = total

    vmem = pl.BlockSpec(memory_space=pltpu.VMEM)
    return pl.pallas_call(
        body,
        out_shape=jax.ShapeDtypeStruct((1, rows_here, width_y), jnp.float32),
        in_specs=[vmem] * count,
        out_specs=vmem,
        name="strip_image",
    )


def swap(array, axis, k):
    return lax.ppermute(array, axis, [(i, i ^ k) for i in range(lax.axis_size(axis))])


def far_first(count):
    return sorted(range(1, count), reverse=True)


def by_strips(velocity, initial_field, anchor_x, anchor_y, source_cell, receivers):
    slabs, shots = lax.axis_size("slab"), lax.axis_size("shot")
    window_rows, window_cols = initial_field.shape[2:]
    strip = window_rows // slabs
    records = receivers.shape[1]
    packed = strip_pack(window_rows, window_cols, slabs, strip)(anchor_x, anchor_y, velocity, initial_field)
    held = list(packed)
    for k in far_first(slabs):
        held[k] = swap(packed[k], "slab", k)
    parts = strip_steps(window_rows, window_cols, slabs, strip, records)(
        anchor_x, anchor_y, source_cell, receivers, *held
    )
    back = list(parts)
    for k in far_first(slabs):
        back[k] = swap(parts[k], "slab", k)
    traces, same, other = strip_gather(window_rows, window_cols, slabs, shots, strip, records)(
        anchor_x, anchor_y, *back
    )
    shares = [same] + [swap(other if k % 2 else same, "shot", k) for k in (3, 2, 1)]
    image = strip_image(window_rows, window_cols, velocity.shape[2], velocity.shape[1] // shots, shots)(*shares)
    return (traces, image)


def strips_fit(mesh, velocity, initial_field, receivers):
    slabs, shots = mesh.shape["slab"], mesh.shape["shot"]
    layers, width_x, width_y = velocity.shape
    shot_count, levels, window_rows, window_cols = initial_field.shape
    records = receivers.shape[1]
    return (
        layers == levels == slabs
        and slabs in (2, 4, 8)
        and shot_count == shots == 4
        and width_x == 2 * window_rows
        and width_y == 2 * window_cols
        and window_rows % (slabs * SUBLANES) == 0
        and (window_rows // 2) % (window_rows // slabs) == 0
        and window_rows // slabs + 2 * STEPS <= window_rows
        and window_cols % LANES == 0
        and records % (2 * LANES) == 0
        and (2 * STEPS) % SUBLANES == 0
    )


def solution(mesh):
    placed = (
        P("slab", None, None),
        P("shot", "slab", None, None),
        P("shot"),
        P("shot"),
        P("shot"),
        P("shot", None),
    )

    def whole(velocity, initial_field, anchor_x, anchor_y, source_cell, receivers):
        fit = strips_fit(mesh, velocity, initial_field, receivers)
        return jax.shard_map(
            by_strips if fit else by_depth,
            mesh=mesh,
            in_specs=placed,
            out_specs=(P("shot", None, None), P("slab", "shot", None)),
            check_vma=False,
        )(velocity, initial_field, anchor_x, anchor_y, source_cell, receivers)

    return whole
```

```python
import math

import jax
import jax.numpy as jnp
from jax import lax
from jax.experimental import pallas as pl
from jax.experimental.pallas import tpu as pltpu
from jax.sharding import PartitionSpec as P

STEPS = 4


COURANT = 0.125
AMPLITUDE = 4.0

SUBLANES = 8
LANES = 128
VMEM_LIMIT = 16 * 1024 * 1024


def wavelet(instant):
    shifted = 0.8 * (instant - 1.5)
    return (1.0 - 2.0 * shifted * shifted) * math.exp(-shifted * shifted)


def with_halo(cells, sides, width):
    for axis, dim in sides:
        count = lax.axis_size(axis)
        ends = count - 1
        head = lax.slice_in_dim(cells, 0, width, axis=dim)
        tail = lax.slice_in_dim(cells, cells.shape[dim] - width, cells.shape[dim], axis=dim)
        cells = jnp.concatenate(
            [
                lax.ppermute(tail, axis, [(i, (i + 1) % count) for i in range(ends)]),
                cells,
                lax.ppermute(head, axis, [((i + 1) % count, i) for i in range(ends)]),
            ],
            axis=dim,
        )
    return cells


def propagate(speed, field, extend, source, depth_start):
    coefficient = jnp.square(COURANT * speed)
    column_count = speed.shape[3]
    depth_place = lax.broadcasted_iota(jnp.int32, speed.shape, 1) + depth_start
    row_place = lax.broadcasted_iota(jnp.int32, speed.shape, 2)
    column_place = lax.broadcasted_iota(jnp.int32, speed.shape, 3)
    source_row = (source // column_count)[:, None, None, None]
    source_column = (source % column_count)[:, None, None, None]
    struck = (depth_place == 1) & (row_place == source_row) & (column_place == source_column)
    source_term = jnp.where(struck, coefficient, jnp.float32(0.0))
    previous = field
    current = field
    energy = jnp.zeros(speed.shape, jnp.float32)
    surfaces = []
    for instant in range(STEPS):
        padded = extend(current)
        laplacian = padded[:, 2:, 1:-1, 1:-1] + padded[:, :-2, 1:-1, 1:-1]
        laplacian = laplacian + padded[:, 1:-1, 2:, 1:-1] + padded[:, 1:-1, :-2, 1:-1]
        laplacian = laplacian + padded[:, 1:-1, 1:-1, 2:] + padded[:, 1:-1, 1:-1, :-2]
        laplacian = laplacian - 6.0 * current
        advanced = 2.0 * current - previous + coefficient * laplacian
        advanced = advanced + source_term * (AMPLITUDE * wavelet(instant))
        energy = energy + advanced * advanced
        surfaces.append(advanced[:, 0])
        previous, current = (current, advanced)
    return (energy / STEPS, jnp.stack(surfaces, axis=1))


def by_depth(velocity, initial_field, anchor_x, anchor_y, source_cell, receivers):
    slab_index = lax.axis_index("slab")
    layers, width_x, width_y = velocity.shape
    shot_count = initial_field.shape[0]
    window_rows = initial_field.shape[2]
    window_cols = initial_field.shape[3]

    def cut_window(start_x, start_y):
        return lax.dynamic_slice(
            velocity, (jnp.int32(0), start_x, start_y), (layers, window_rows, window_cols)
        )

    windows = jax.vmap(cut_window)(anchor_x, anchor_y)
    depth_start = slab_index * layers

    def extend_depth(current):
        rimmed = with_halo(current, (("slab", 1),), 1)
        return jnp.pad(rimmed, ((0, 0), (0, 0), (1, 1), (1, 1)))

    energy_here, surface = propagate(windows, initial_field, extend_depth, source_cell, depth_start)
    local_rows = surface.shape[2]
    receiver_row = receivers // window_cols
    receiver_column = receivers % window_cols
    holds = (receiver_row >= 0) & (receiver_row < local_rows) & (depth_start == 0)
    flat_local = jnp.clip(receiver_row, 0, local_rows - 1) * window_cols + receiver_column
    record_count = receivers.shape[1]
    picked = jnp.take_along_axis(
        surface.reshape(shot_count, STEPS, -1),
        jnp.broadcast_to(flat_local[:, None, :], (shot_count, STEPS, record_count)),
        axis=2,
    )
    picked = jnp.where(holds[:, None, :], picked, jnp.float32(0.0))
    traces = lax.psum(picked, "slab")
    partial_image = jnp.zeros((layers, width_x, width_y), jnp.float32)
    corner = (jnp.int32(0), anchor_x[0], anchor_y[0])
    partial_image = lax.dynamic_update_slice(partial_image, energy_here[0], corner)
    summed = lax.psum_scatter(partial_image, "shot", scatter_dimension=1, tiled=True)
    return (traces, summed)


def small_vmem(name, **options):
    return dict(compiler_params=pltpu.CompilerParams(vmem_limit_bytes=VMEM_LIMIT, **options), name=name)


def strip_of(place, slabs):
    return place % 2 * (slabs // 2) + place // 2


def strip_pack(window_rows, window_cols, slabs, strip):
    tall = strip + 2 * STEPS

    def body(anchor_x, anchor_y, velocity, field, *rest):
        blocks, (corner, speed, pressure, planes, sems) = rest[:slabs], rest[slabs:]
        mine = lax.axis_index("slab")
        copies = [
            pltpu.make_async_copy(anchor_x, corner.at[0], sems.at[0]),
            pltpu.make_async_copy(anchor_y, corner.at[1], sems.at[1]),
            pltpu.make_async_copy(field.at[0, 0], pressure, sems.at[2]),
            pltpu.make_async_copy(velocity.at[0], speed, sems.at[3]),
        ]
        for copy in copies:
            copy.start()
        for copy in copies[:3]:
            copy.wait()
        top, left = corner[0, 0], corner[1, 0]
        rolled = pltpu.roll(pressure[...], left % window_cols, axis=1)
        rolled = pltpu.roll(rolled, (top + STEPS) % window_rows, axis=0)
        planes[0, :window_rows] = rolled
        planes[0, window_rows:] = rolled[: 2 * STEPS]
        copies[3].wait()
        rows = lax.broadcasted_iota(jnp.int32, (window_rows, window_cols), 0)
        columns = lax.broadcasted_iota(jnp.int32, (window_rows, window_cols), 1)
        near = jnp.where(columns >= left, speed[:window_rows, :window_cols], speed[:window_rows, window_cols:])
        far = jnp.where(columns >= left, speed[window_rows:, :window_cols], speed[window_rows:, window_cols:])
        chosen = COURANT * jnp.where(rows >= top, near, far)
        coefficient = pltpu.roll(chosen * chosen, STEPS, axis=0)
        planes[1, :window_rows] = coefficient
        planes[1, window_rows:] = coefficient[: 2 * STEPS]
        for k in range(slabs):
            start = pl.multiple_of(strip_of(mine ^ k, slabs) * strip, SUBLANES)
            blocks[k][:tall] = planes[0, pl.ds(start, tall), :]
            blocks[k][tall:] = planes[1, pl.ds(start, tall), :]

    hbm = pl.BlockSpec(memory_space=pl.ANY)
    vmem = pl.BlockSpec(memory_space=pltpu.VMEM)
    return pl.pallas_call(
        body,
        out_shape=[jax.ShapeDtypeStruct((2 * tall, window_cols), jnp.float32)] * slabs,
        in_specs=[hbm] * 4,
        out_specs=[vmem] * slabs,
        scratch_shapes=[
            pltpu.SMEM((2, 1), jnp.int32),
            pltpu.VMEM((2 * window_rows, 2 * window_cols), jnp.float32),
            pltpu.VMEM((window_rows, window_cols), jnp.float32),
            pltpu.VMEM((2, window_rows + 2 * STEPS, window_cols), jnp.float32),
            pltpu.SemaphoreType.DMA((4,)),
        ],
        **small_vmem("strip_pack"),
    )


def strip_steps(window_rows, window_cols, slabs, strip, records):
    tall = strip + 2 * STEPS
    pieces = window_cols // LANES

    def body(anchor_x, anchor_y, source, receivers, *rest):
        blocks, (same, other, heard), (fields, speeds, energy, surface) = (
            rest[:slabs],
            rest[slabs : slabs + 3],
            rest[slabs + 3 :],
        )
        mine = lax.axis_index("slab")
        core = lax.axis_index("shot") % 2
        top, left = anchor_x[0], anchor_y[0]
        for k in range(slabs):
            fields[0, mine ^ k] = blocks[k][:tall]
            speeds[mine ^ k] = blocks[k][tall:]
        rows = lax.broadcasted_iota(jnp.int32, (tall, window_cols), 0)
        columns = lax.broadcasted_iota(jnp.int32, (tall, window_cols), 1)
        begin = strip_of(mine, slabs) * strip - STEPS

        def local_row(row):
            return (row + top - begin + window_rows) % window_rows

        def local_column(column):
            return (column + left) % window_cols

        inside_up = rows != local_row(0)
        inside_down = rows != local_row(window_rows - 1)
        inside_left = columns != local_column(0)
        inside_right = columns != local_column(window_cols - 1)
        struck = (rows == local_row(source[0] // window_cols)) & (columns == local_column(source[0] % window_cols))
        source_term = jnp.where(struck, speeds[1], 0.0)
        for instant in range(STEPS):
            now, then = instant % 2, (instant + 1) % 2
            for level in range(slabs):
                current = fields[now, level]
                previous = fields[then if instant else now, level]
                laplacian = jnp.where(inside_up, pltpu.roll(current, 1, axis=0), 0.0)
                laplacian = laplacian + jnp.where(inside_down, pltpu.roll(current, tall - 1, axis=0), 0.0)
                laplacian = laplacian + jnp.where(inside_left, pltpu.roll(current, 1, axis=1), 0.0)
                laplacian = laplacian + jnp.where(inside_right, pltpu.roll(current, window_cols - 1, axis=1), 0.0)
                if level > 0:
                    laplacian = laplacian + fields[now, level - 1]
                if level < slabs - 1:
                    laplacian = laplacian + fields[now, level + 1]
                laplacian = laplacian - 6.0 * current
                advanced = 2.0 * current - previous + speeds[level] * laplacian
                if level == 1:
                    advanced = advanced + source_term * (AMPLITUDE * wavelet(instant))
                if level == 0:
                    surface[instant * tall : (instant + 1) * tall] = advanced
                if instant < STEPS - 1:
                    fields[then, level] = advanced
                square = advanced * advanced
                energy[level] = square if instant == 0 else energy[level] + square
        for out, parity in ((same, core), (other, 1 - core)):
            for pair in range(slabs // 2):
                for i in range(pieces):
                    at = (pair * pieces + i) * strip
                    out[at : at + strip] = (
                        energy[2 * pair + parity, STEPS : STEPS + strip, i * LANES : (i + 1) * LANES] / STEPS
                    )
            tags = lax.broadcasted_iota(jnp.int32, (SUBLANES, LANES), 0)
            out[slabs // 2 * pieces * strip :] = jnp.where(tags == 0, top, left).astype(jnp.float32)
        row = (receivers[...] // window_cols + top) % window_rows - begin
        column = (receivers[...] % window_cols + left) % window_cols
        row = jnp.where((row >= STEPS) & (row < STEPS + strip), row, -1)
        cells = lax.broadcasted_iota(jnp.int32, (window_cols, records), 0)
        chosen = jnp.where(cells == column, 1.0, 0.0)
        picked = jnp.dot(surface[...], chosen, precision=lax.Precision.HIGHEST, preferred_element_type=jnp.float32)
        places = lax.broadcasted_iota(jnp.int32, (tall, records), 0)
        for n in range(STEPS):
            own = jnp.where(places == row, picked[n * tall : (n + 1) * tall], 0.0)
            own = jnp.sum(own, axis=0, keepdims=True)
            for i in range(records // LANES):
                heard[i * STEPS + n : i * STEPS + n + 1] = own[:, i * LANES : (i + 1) * LANES]

    smem = pl.BlockSpec(memory_space=pltpu.SMEM)
    vmem = pl.BlockSpec(memory_space=pltpu.VMEM)
    share = jax.ShapeDtypeStruct((slabs // 2 * pieces * strip + SUBLANES, LANES), jnp.float32)
    return pl.pallas_call(
        body,
        out_shape=[share, share, jax.ShapeDtypeStruct((records // LANES * STEPS, LANES), jnp.float32)],
        in_specs=[smem, smem, smem, vmem] + [vmem] * slabs,
        out_specs=[vmem] * 3,
        scratch_shapes=[
            pltpu.VMEM((2, slabs, tall, window_cols), jnp.float32),
            pltpu.VMEM((slabs, tall, window_cols), jnp.float32),
            pltpu.VMEM((slabs, tall, window_cols), jnp.float32),
            pltpu.VMEM((STEPS * tall, window_cols), jnp.float32),
        ],
        **small_vmem("strip_steps"),
    )


def strip_sum(window_rows, window_cols, width_y, rows_here, slabs, shots, strip, records):
    pieces = window_cols // LANES
    wide = width_y // LANES
    pairs = slabs // 2
    heard_rows = records // LANES * STEPS

    def body(heard, heard_too, *rest):
        blocks, outs = rest[:shots], rest[shots:]
        mine = lax.axis_index("slab")
        zone = mine // 2
        first = lax.axis_index("shot") * rows_here + zone * strip
        rows = lax.broadcasted_iota(jnp.int32, (strip, LANES), 0) + first
        columns = lax.broadcasted_iota(jnp.int32, (strip, LANES), 1)
        insides = []
        for block in blocks:
            tag = block[pairs * pieces * strip :].astype(jnp.int32)
            down = rows - tag[0:1]
            tall = (down >= 0) & (down < window_rows)
            along = columns - tag[1:2]
            insides.append([tall & (along >= -i * LANES) & (along < window_cols - i * LANES) for i in range(wide)])
        for k in range(pairs):
            pair = zone ^ k
            for i in range(wide):
                start = pl.multiple_of((pair * pieces + i % pieces) * strip, SUBLANES)
                total = jnp.zeros((strip, LANES), jnp.float32)
                for block, inside in zip(blocks, insides):
                    total = total + jnp.where(inside[i], block[pl.ds(start, strip), :], 0.0)
                outs[k][i * strip : (i + 1) * strip] = total
            outs[k][wide * strip :] = heard[...] + heard_too[...]

    vmem = pl.BlockSpec(memory_space=pltpu.VMEM)
    return pl.pallas_call(
        body,
        out_shape=[jax.ShapeDtypeStruct((wide * strip + heard_rows, LANES), jnp.float32)] * pairs,
        in_specs=[vmem] * (2 + shots),
        out_specs=[vmem] * pairs,
        **small_vmem("strip_sum"),
    )


def strip_place(width_y, rows_here, slabs, strip, records):
    wide = width_y // LANES
    pairs = slabs // 2

    def body(*rest):
        blocks, (traces, image) = rest[:pairs], rest[pairs:]
        zone = lax.axis_index("slab") // 2
        for k in range(pairs):
            start = pl.multiple_of((zone ^ k) * strip, SUBLANES)
            for i in range(wide):
                image[0, pl.ds(start, strip), i * LANES : (i + 1) * LANES] = blocks[k][i * strip : (i + 1) * strip]
        total = blocks[0][wide * strip :]
        for k in range(1, pairs):
            total = total + blocks[k][wide * strip :]
        for i in range(records // LANES):
            traces[0, :, i * LANES : (i + 1) * LANES] = total[i * STEPS : (i + 1) * STEPS]

    vmem = pl.BlockSpec(memory_space=pltpu.VMEM)
    return pl.pallas_call(
        body,
        out_shape=[
            jax.ShapeDtypeStruct((1, STEPS, records), jnp.float32),
            jax.ShapeDtypeStruct((1, rows_here, width_y), jnp.float32),
        ],
        in_specs=[vmem] * pairs,
        out_specs=[vmem] * 2,
        **small_vmem("strip_place"),
    )


def swap(array, axis, k):
    return lax.ppermute(array, axis, [(i, i ^ k) for i in range(lax.axis_size(axis))])


def far_first(count):
    return sorted(range(1, count), reverse=True)


def hand_over(array, over_x, flip):
    slabs, shots = lax.axis_size("slab"), lax.axis_size("shot")
    pairs = []
    for place in range(slabs):
        for shot in range(shots):
            side, core = place % 2, shot % 2
            to_place = place - side + (core ^ flip)
            to_shot = ((shot // 2) ^ over_x) * 2 + side
            pairs.append((place * shots + shot, to_place * shots + to_shot))
    return lax.ppermute(array, ("slab", "shot"), pairs)


def by_strips(velocity, initial_field, anchor_x, anchor_y, source_cell, receivers):
    slabs, shots = lax.axis_size("slab"), lax.axis_size("shot")
    window_rows, window_cols = initial_field.shape[2:]
    width_y = velocity.shape[2]
    rows_here = velocity.shape[1] // shots
    strip = window_rows // slabs
    records = receivers.shape[1]
    packed = strip_pack(window_rows, window_cols, slabs, strip)(anchor_x, anchor_y, velocity, initial_field)
    held = list(packed)
    for k in far_first(slabs):
        held[k] = swap(packed[k], "slab", k)
    same, other, heard = strip_steps(window_rows, window_cols, slabs, strip, records)(
        anchor_x, anchor_y, source_cell, receivers, *held
    )
    shares = [hand_over(other if flip else same, over_x, flip) for over_x in (1, 0) for flip in (1, 0)]
    heard_too = swap(heard, "slab", 1)
    sums = strip_sum(window_rows, window_cols, width_y, rows_here, slabs, shots, strip, records)(
        heard, heard_too, *shares
    )
    back = list(sums)
    for k in far_first(slabs // 2):
        back[k] = swap(sums[k], "slab", 2 * k)
    traces, image = strip_place(width_y, rows_here, slabs, strip, records)(*back)
    return (traces, image)


def strips_fit(mesh, velocity, initial_field, receivers):
    slabs, shots = mesh.shape["slab"], mesh.shape["shot"]
    layers, width_x, width_y = velocity.shape
    shot_count, levels, window_rows, window_cols = initial_field.shape
    records = receivers.shape[1]
    return (
        layers == levels == slabs
        and slabs in (2, 4, 8)
        and shot_count == shots == 4
        and width_x == 2 * window_rows
        and width_y == 2 * window_cols
        and window_rows % (slabs * SUBLANES) == 0
        and width_x // shots == window_rows // 2
        and window_rows // slabs + 2 * STEPS <= window_rows
        and window_cols % LANES == 0
        and records % (2 * LANES) == 0
        and (2 * STEPS) % SUBLANES == 0
    )


def solution(mesh):
    placed = (
        P("slab", None, None),
        P("shot", "slab", None, None),
        P("shot"),
        P("shot"),
        P("shot"),
        P("shot", None),
    )

    def whole(velocity, initial_field, anchor_x, anchor_y, source_cell, receivers):
        fit = strips_fit(mesh, velocity, initial_field, receivers)
        return jax.shard_map(
            by_strips if fit else by_depth,
            mesh=mesh,
            in_specs=placed,
            out_specs=(P("shot", None, None), P("slab", "shot", None)),
            check_vma=False,
        )(velocity, initial_field, anchor_x, anchor_y, source_cell, receivers)

    return whole
```

```python
import math

import jax
import jax.numpy as jnp
from jax import lax
from jax.experimental import pallas as pl
from jax.experimental.pallas import tpu as pltpu
from jax.sharding import PartitionSpec as P

STEPS = 4


COURANT = 0.125
AMPLITUDE = 4.0

SUBLANES = 8
LANES = 128
VMEM_LIMIT = 16 * 1024 * 1024


def wavelet(instant):
    shifted = 0.8 * (instant - 1.5)
    return (1.0 - 2.0 * shifted * shifted) * math.exp(-shifted * shifted)


def with_halo(cells, sides, width):
    for axis, dim in sides:
        count = lax.axis_size(axis)
        ends = count - 1
        head = lax.slice_in_dim(cells, 0, width, axis=dim)
        tail = lax.slice_in_dim(cells, cells.shape[dim] - width, cells.shape[dim], axis=dim)
        cells = jnp.concatenate(
            [
                lax.ppermute(tail, axis, [(i, (i + 1) % count) for i in range(ends)]),
                cells,
                lax.ppermute(head, axis, [((i + 1) % count, i) for i in range(ends)]),
            ],
            axis=dim,
        )
    return cells


def propagate(speed, field, extend, source, depth_start):
    coefficient = jnp.square(COURANT * speed)
    column_count = speed.shape[3]
    depth_place = lax.broadcasted_iota(jnp.int32, speed.shape, 1) + depth_start
    row_place = lax.broadcasted_iota(jnp.int32, speed.shape, 2)
    column_place = lax.broadcasted_iota(jnp.int32, speed.shape, 3)
    source_row = (source // column_count)[:, None, None, None]
    source_column = (source % column_count)[:, None, None, None]
    struck = (depth_place == 1) & (row_place == source_row) & (column_place == source_column)
    source_term = jnp.where(struck, coefficient, jnp.float32(0.0))
    previous = field
    current = field
    energy = jnp.zeros(speed.shape, jnp.float32)
    surfaces = []
    for instant in range(STEPS):
        padded = extend(current)
        laplacian = padded[:, 2:, 1:-1, 1:-1] + padded[:, :-2, 1:-1, 1:-1]
        laplacian = laplacian + padded[:, 1:-1, 2:, 1:-1] + padded[:, 1:-1, :-2, 1:-1]
        laplacian = laplacian + padded[:, 1:-1, 1:-1, 2:] + padded[:, 1:-1, 1:-1, :-2]
        laplacian = laplacian - 6.0 * current
        advanced = 2.0 * current - previous + coefficient * laplacian
        advanced = advanced + source_term * (AMPLITUDE * wavelet(instant))
        energy = energy + advanced * advanced
        surfaces.append(advanced[:, 0])
        previous, current = (current, advanced)
    return (energy / STEPS, jnp.stack(surfaces, axis=1))


def by_depth(velocity, initial_field, anchor_x, anchor_y, source_cell, receivers):
    slab_index = lax.axis_index("slab")
    layers, width_x, width_y = velocity.shape
    shot_count = initial_field.shape[0]
    window_rows = initial_field.shape[2]
    window_cols = initial_field.shape[3]

    def cut_window(start_x, start_y):
        return lax.dynamic_slice(
            velocity, (jnp.int32(0), start_x, start_y), (layers, window_rows, window_cols)
        )

    windows = jax.vmap(cut_window)(anchor_x, anchor_y)
    depth_start = slab_index * layers

    def extend_depth(current):
        rimmed = with_halo(current, (("slab", 1),), 1)
        return jnp.pad(rimmed, ((0, 0), (0, 0), (1, 1), (1, 1)))

    energy_here, surface = propagate(windows, initial_field, extend_depth, source_cell, depth_start)
    local_rows = surface.shape[2]
    receiver_row = receivers // window_cols
    receiver_column = receivers % window_cols
    holds = (receiver_row >= 0) & (receiver_row < local_rows) & (depth_start == 0)
    flat_local = jnp.clip(receiver_row, 0, local_rows - 1) * window_cols + receiver_column
    record_count = receivers.shape[1]
    picked = jnp.take_along_axis(
        surface.reshape(shot_count, STEPS, -1),
        jnp.broadcast_to(flat_local[:, None, :], (shot_count, STEPS, record_count)),
        axis=2,
    )
    picked = jnp.where(holds[:, None, :], picked, jnp.float32(0.0))
    traces = lax.psum(picked, "slab")
    partial_image = jnp.zeros((layers, width_x, width_y), jnp.float32)
    corner = (jnp.int32(0), anchor_x[0], anchor_y[0])
    partial_image = lax.dynamic_update_slice(partial_image, energy_here[0], corner)
    summed = lax.psum_scatter(partial_image, "shot", scatter_dimension=1, tiled=True)
    return (traces, summed)


def small_vmem(name, **options):
    return dict(compiler_params=pltpu.CompilerParams(vmem_limit_bytes=VMEM_LIMIT, **options), name=name)


def strip_of(place, slabs):
    return place % 2 * (slabs // 2) + place // 2


def strip_pack(window_rows, window_cols, slabs, strip, records):
    tall = strip + 2 * STEPS

    def body(anchor_x, anchor_y, receivers, velocity, field, *rest):
        blocks, (facts, listed, speed, pressure, planes, sems) = rest[:slabs], rest[slabs:]
        mine = lax.axis_index("slab")
        copies = [
            pltpu.make_async_copy(field.at[0, 0], pressure, sems.at[0]),
            pltpu.make_async_copy(velocity.at[0], speed, sems.at[1]),
            pltpu.make_async_copy(receivers, listed, sems.at[2]),
        ]
        for copy in copies:
            copy.start()
        top, left = anchor_x[0], anchor_y[0]
        kinds = lax.broadcasted_iota(jnp.int32, facts.shape, 0)
        facts[...] = jnp.where(kinds == 0, top, left)
        copies[0].wait()
        rolled = pltpu.roll(pressure[...], left % window_cols, axis=1)
        rolled = pltpu.roll(rolled, (top + STEPS) % window_rows, axis=0)
        planes[0, :window_rows] = rolled
        planes[0, window_rows:] = rolled[: 2 * STEPS]
        copies[1].wait()
        rows = lax.broadcasted_iota(jnp.int32, (window_rows, window_cols), 0)
        columns = lax.broadcasted_iota(jnp.int32, (window_rows, window_cols), 1)
        near = jnp.where(columns >= left, speed[:window_rows, :window_cols], speed[:window_rows, window_cols:])
        far = jnp.where(columns >= left, speed[window_rows:, :window_cols], speed[window_rows:, window_cols:])
        chosen = COURANT * jnp.where(rows >= top, near, far)
        coefficient = pltpu.roll(chosen * chosen, STEPS, axis=0)
        planes[1, :window_rows] = coefficient
        planes[1, window_rows:] = coefficient[: 2 * STEPS]
        for k in range(slabs):
            start = pl.multiple_of(strip_of(mine ^ k, slabs) * strip, SUBLANES)
            blocks[k][:tall] = planes[0, pl.ds(start, tall), :]
            blocks[k][tall:] = planes[1, pl.ds(start, tall), :]
        copies[2].wait()

    hbm = pl.BlockSpec(memory_space=pltpu.HBM)
    smem = pl.BlockSpec(memory_space=pltpu.SMEM)
    vmem = pl.BlockSpec(memory_space=pltpu.VMEM)
    return pl.pallas_call(
        body,
        out_shape=[jax.ShapeDtypeStruct((2 * tall, window_cols), jnp.float32)] * slabs
        + [
            jax.ShapeDtypeStruct((SUBLANES, window_cols), jnp.int32),
            jax.ShapeDtypeStruct((1, records), jnp.int32),
        ],
        in_specs=[smem, smem] + [hbm] * 3,
        out_specs=[vmem] * (slabs + 2),
        scratch_shapes=[
            pltpu.VMEM((2 * window_rows, 2 * window_cols), jnp.float32),
            pltpu.VMEM((window_rows, window_cols), jnp.float32),
            pltpu.VMEM((2, window_rows + 2 * STEPS, window_cols), jnp.float32),
            pltpu.SemaphoreType.DMA((3,)),
        ],
        **small_vmem("strip_pack"),
    )


def strip_steps(window_rows, window_cols, slabs, strip, records, order, zones):
    tall = strip + 2 * STEPS
    pieces = window_cols // LANES
    deep = len(zones) * pieces * strip

    def body(source, facts, receivers, *rest):
        blocks, outs = dict(zip(order, rest)), rest[slabs : slabs + 2]
        fields, speeds, energy, surface = rest[slabs + 2 :]
        mine = lax.axis_index("slab")
        core = lax.axis_index("shot") % 2
        top, left = facts[0:1], facts[1:2]
        for k in range(slabs):
            fields[0, mine ^ k] = blocks[k][:tall]
            speeds[mine ^ k] = blocks[k][tall:]
        rows = lax.broadcasted_iota(jnp.int32, (tall, window_cols), 0)
        columns = lax.broadcasted_iota(jnp.int32, (tall, window_cols), 1)
        begin = strip_of(mine, slabs) * strip - STEPS

        def local_row(row):
            return (row + top - begin + window_rows) % window_rows

        def local_column(column):
            return (column + left) % window_cols

        inside_up = rows != local_row(0)
        inside_down = rows != local_row(window_rows - 1)
        inside_left = columns != local_column(0)
        inside_right = columns != local_column(window_cols - 1)
        struck = (rows == local_row(source[0] // window_cols)) & (columns == local_column(source[0] % window_cols))
        source_term = jnp.where(struck, speeds[1], 0.0)
        for instant in range(STEPS):
            now, then = instant % 2, (instant + 1) % 2
            for level in range(slabs):
                current = fields[now, level]
                previous = fields[then if instant else now, level]
                laplacian = jnp.where(inside_up, pltpu.roll(current, 1, axis=0), 0.0)
                laplacian = laplacian + jnp.where(inside_down, pltpu.roll(current, tall - 1, axis=0), 0.0)
                laplacian = laplacian + jnp.where(inside_left, pltpu.roll(current, 1, axis=1), 0.0)
                laplacian = laplacian + jnp.where(inside_right, pltpu.roll(current, window_cols - 1, axis=1), 0.0)
                if level > 0:
                    laplacian = laplacian + fields[now, level - 1]
                if level < slabs - 1:
                    laplacian = laplacian + fields[now, level + 1]
                laplacian = laplacian - 6.0 * current
                advanced = 2.0 * current - previous + speeds[level] * laplacian
                if level == 1:
                    advanced = advanced + source_term * (AMPLITUDE * wavelet(instant))
                if level == 0:
                    surface[instant * tall : (instant + 1) * tall] = advanced
                if instant < STEPS - 1:
                    fields[then, level] = advanced
                square = advanced * advanced
                energy[level] = square if instant == 0 else energy[level] + square
        for out, parity in zip(outs, (core, 1 - core)):
            for j, k in enumerate(zones):
                level = 2 * ((mine // 2) ^ k) + parity
                for i in range(pieces):
                    at = (j * pieces + i) * strip
                    out[at : at + strip] = energy[level, STEPS : STEPS + strip, i * LANES : (i + 1) * LANES] / STEPS
            out[deep : deep + SUBLANES] = facts[:, :LANES].astype(jnp.float32)
        row = (receivers[...] // window_cols + top[:, :1]) % window_rows - begin
        column = (receivers[...] % window_cols + left[:, :1]) % window_cols
        row = jnp.where((row >= STEPS) & (row < STEPS + strip), row, -1)
        cells = lax.broadcasted_iota(jnp.int32, (window_cols, records), 0)
        chosen = jnp.where(cells == column, 1.0, 0.0)
        picked = jnp.dot(surface[...], chosen, precision=lax.Precision.HIGHEST, preferred_element_type=jnp.float32)
        places = lax.broadcasted_iota(jnp.int32, (tall, records), 0)
        for n in range(STEPS):
            own = jnp.where(places == row, picked[n * tall : (n + 1) * tall], 0.0)
            own = jnp.sum(own, axis=0, keepdims=True)
            for i in range(records // LANES):
                at = deep + SUBLANES + i * STEPS + n
                for out in outs:
                    out[at : at + 1] = own[:, i * LANES : (i + 1) * LANES]

    vmem = pl.BlockSpec(memory_space=pltpu.VMEM)
    return pl.pallas_call(
        body,
        out_shape=[jax.ShapeDtypeStruct((deep + SUBLANES + records // LANES * STEPS, LANES), jnp.float32)] * 2,
        in_specs=[pl.BlockSpec(memory_space=pltpu.SMEM)] + [vmem] * (2 + slabs),
        out_specs=[vmem] * 2,
        scratch_shapes=[
            pltpu.VMEM((2, slabs, tall, window_cols), jnp.float32),
            pltpu.VMEM((slabs, tall, window_cols), jnp.float32),
            pltpu.VMEM((slabs, tall, window_cols), jnp.float32),
            pltpu.VMEM((STEPS * tall, window_cols), jnp.float32),
        ],
        **small_vmem("strip_steps"),
    )


def strip_share(window_rows, window_cols, width_y, rows_here, strip, records, chunks):
    pieces = window_cols // LANES
    wide = width_y // LANES
    deep = sum(len(chunk) for chunk in chunks) * pieces * strip
    heard_rows = records // LANES * STEPS

    def body(keep, got, *outs):
        mine, shot = lax.axis_index("slab"), lax.axis_index("shot")
        zone, side = mine // 2, mine % 2
        shares = (keep, got)
        tags = [share[deep : deep + SUBLANES].astype(jnp.int32) for share in shares]
        columns = lax.broadcasted_iota(jnp.int32, (strip, LANES), 1)
        for over_x in (1, 0):
            to_shot = ((shot // 2) ^ over_x) * 2 + side
            rows = lax.broadcasted_iota(jnp.int32, (strip, LANES), 0) + to_shot * rows_here + zone * strip
            insides = []
            for tag in tags:
                down, along = rows - tag[0:1], columns - tag[1:2]
                tall = (down >= 0) & (down < window_rows)
                insides.append(
                    [tall & (along >= -i * LANES) & (along < window_cols - i * LANES) for i in range(wide)]
                )
            first = 0
            for c, chunk in enumerate(chunks):
                out = outs[(1 - over_x) * len(chunks) + c]
                for j in range(len(chunk)):
                    for i in range(wide):
                        start = ((first + j) * pieces + i % pieces) * strip
                        parts = [
                            jnp.where(inside[i], share[start : start + strip], 0.0)
                            for share, inside in zip(shares, insides)
                        ]
                        at = (j * wide + i) * strip
                        out[at : at + strip] = parts[0] + parts[1]
                first += len(chunk)
        heard, told = outs[2 * len(chunks) :]
        same_core = shot % 2 == side
        heard[...] = jnp.where(same_core, keep[deep + SUBLANES :], got[deep + SUBLANES :])
        told[...] = jnp.where(same_core, got[deep + SUBLANES :], keep[deep + SUBLANES :])

    vmem = pl.BlockSpec(memory_space=pltpu.VMEM)
    sizes = [len(chunk) * wide * strip for chunk in chunks]
    return pl.pallas_call(
        body,
        out_shape=[jax.ShapeDtypeStruct((size, LANES), jnp.float32) for size in sizes + sizes + [heard_rows] * 2],
        in_specs=[vmem] * 2,
        out_specs=[vmem] * (2 * len(chunks) + 2),
        **small_vmem("strip_share"),
    )


def strip_sum(width_y, strip, records, count):
    deep = width_y // LANES * strip
    heard_rows = records // LANES * STEPS

    def body(come, own, heard_too, heard, *outs):
        for j, out in enumerate(outs):
            out[:deep] = own[j * deep : (j + 1) * deep] + come[j * deep : (j + 1) * deep]
            out[deep:] = heard[...] + heard_too[...]

    vmem = pl.BlockSpec(memory_space=pltpu.VMEM)
    return pl.pallas_call(
        body,
        out_shape=[jax.ShapeDtypeStruct((deep + heard_rows, LANES), jnp.float32)] * count,
        in_specs=[vmem] * 4,
        out_specs=[vmem] * count,
        **small_vmem("strip_sum"),
    )


def strip_place(width_y, rows_here, slabs, strip, records, order):
    wide = width_y // LANES
    pairs = slabs // 2

    def body(*rest):
        blocks, (traces, image) = dict(zip(order, rest)), rest[pairs:]
        zone = lax.axis_index("slab") // 2
        for k in range(pairs):
            start = pl.multiple_of((zone ^ k) * strip, SUBLANES)
            for i in range(wide):
                image[0, pl.ds(start, strip), i * LANES : (i + 1) * LANES] = blocks[k][i * strip : (i + 1) * strip]
        total = blocks[0][wide * strip :]
        for k in range(1, pairs):
            total = total + blocks[k][wide * strip :]
        for i in range(records // LANES):
            traces[0, :, i * LANES : (i + 1) * LANES] = total[i * STEPS : (i + 1) * STEPS]

    vmem = pl.BlockSpec(memory_space=pltpu.VMEM)
    return pl.pallas_call(
        body,
        out_shape=[
            jax.ShapeDtypeStruct((1, STEPS, records), jnp.float32),
            jax.ShapeDtypeStruct((1, rows_here, width_y), jnp.float32),
        ],
        in_specs=[vmem] * pairs,
        out_specs=[vmem] * 2,
        **small_vmem("strip_place"),
    )


def swap(array, axis, k):
    return lax.ppermute(array, axis, [(i, i ^ k) for i in range(lax.axis_size(axis))])


def far_first(count):
    return [*range(count // 2, count), *range(count // 2)]


def cross(array, k):
    slabs, shots = lax.axis_size("slab"), lax.axis_size("shot")
    pairs = []
    for place in range(slabs):
        for shot in range(shots):
            side, core = place % 2, shot % 2
            to_place = ((place // 2) ^ k) * 2 + core
            to_shot = shot // 2 * 2 + side
            pairs.append((place * shots + shot, to_place * shots + to_shot))
    return lax.ppermute(array, ("slab", "shot"), pairs)


def by_strips(velocity, initial_field, anchor_x, anchor_y, source_cell, receivers):
    slabs, shots = lax.axis_size("slab"), lax.axis_size("shot")
    window_rows, window_cols = initial_field.shape[2:]
    width_y = velocity.shape[2]
    rows_here = velocity.shape[1] // shots
    strip = window_rows // slabs
    records = receivers.shape[1]
    velocity, initial_field, receivers = (
        pltpu.with_memory_space_constraint(array, pltpu.HBM) for array in (velocity, initial_field, receivers)
    )
    *packed, facts, listed = strip_pack(window_rows, window_cols, slabs, strip, records)(
        anchor_x, anchor_y, receivers, velocity, initial_field
    )
    order = far_first(slabs)
    held = [swap(packed[k], "slab", k) if k else packed[k] for k in order]
    pairs = slabs // 2
    chunks = ((*range(pairs // 2, pairs),), (*range(pairs // 2 - 1, -1, -1),))
    zones = [k for chunk in chunks for k in chunk]
    keep, give = strip_steps(window_rows, window_cols, slabs, strip, records, order, zones)(
        source_cell, facts, listed, *held
    )
    *shares, heard, told = strip_share(window_rows, window_cols, width_y, rows_here, strip, records, chunks)(
        keep, swap(give, "shot", 1)
    )
    come = [swap(share, "shot", 2) for share in shares[: len(chunks)]]
    heard_too = swap(told, "slab", 1)
    back = []
    for c, chunk in enumerate(chunks):
        sums = strip_sum(width_y, strip, records, len(chunk))(come[c], shares[len(chunks) + c], heard_too, heard)
        back += [cross(part, k) for part, k in zip(sums, chunk)]
    traces, image = strip_place(width_y, rows_here, slabs, strip, records, zones)(*back)
    return (traces, image)


def strips_fit(mesh, velocity, initial_field, receivers):
    slabs, shots = mesh.shape["slab"], mesh.shape["shot"]
    layers, width_x, width_y = velocity.shape
    shot_count, levels, window_rows, window_cols = initial_field.shape
    records = receivers.shape[1]
    return (
        layers == levels == slabs
        and slabs in (4, 8)
        and shot_count == shots == 4
        and width_x == 2 * window_rows
        and width_y == 2 * window_cols
        and window_rows % (slabs * SUBLANES) == 0
        and width_x // shots == window_rows // 2
        and window_rows // slabs + 2 * STEPS <= window_rows
        and window_cols % LANES == 0
        and records % (2 * LANES) == 0
        and (2 * STEPS) % SUBLANES == 0
    )


def solution(mesh):
    placed = (
        P("slab", None, None),
        P("shot", "slab", None, None),
        P("shot"),
        P("shot"),
        P("shot"),
        P("shot", None),
    )

    def whole(velocity, initial_field, anchor_x, anchor_y, source_cell, receivers):
        fit = strips_fit(mesh, velocity, initial_field, receivers)
        return jax.shard_map(
            by_strips if fit else by_depth,
            mesh=mesh,
            in_specs=placed,
            out_specs=(P("shot", None, None), P("slab", "shot", None)),
            check_vma=False,
        )(velocity, initial_field, anchor_x, anchor_y, source_cell, receivers)

    return whole
```

```python
import math

import jax
import jax.numpy as jnp
from jax import lax
from jax.experimental import pallas as pl
from jax.experimental.pallas import tpu as pltpu
from jax.sharding import PartitionSpec as P


STEPS = 4


COURANT = 0.125
AMPLITUDE = 4.0

SUBLANES = 8
LANES = 128
VMEM_LIMIT = 16 * 1024 * 1024


def wavelet(instant):
    shifted = 0.8 * (instant - 1.5)
    return (1.0 - 2.0 * shifted * shifted) * math.exp(-shifted * shifted)


def with_halo(cells, sides, width):
    for axis, dim in sides:
        count = lax.axis_size(axis)
        ends = count - 1
        head = lax.slice_in_dim(cells, 0, width, axis=dim)
        tail = lax.slice_in_dim(cells, cells.shape[dim] - width, cells.shape[dim], axis=dim)
        cells = jnp.concatenate(
            [
                lax.ppermute(tail, axis, [(i, (i + 1) % count) for i in range(ends)]),
                cells,
                lax.ppermute(head, axis, [((i + 1) % count, i) for i in range(ends)]),
            ],
            axis=dim,
        )
    return cells


def propagate(speed, field, extend, source, depth_start):
    coefficient = jnp.square(COURANT * speed)
    column_count = speed.shape[3]
    depth_place = lax.broadcasted_iota(jnp.int32, speed.shape, 1) + depth_start
    row_place = lax.broadcasted_iota(jnp.int32, speed.shape, 2)
    column_place = lax.broadcasted_iota(jnp.int32, speed.shape, 3)
    source_row = (source // column_count)[:, None, None, None]
    source_column = (source % column_count)[:, None, None, None]
    struck = (depth_place == 1) & (row_place == source_row) & (column_place == source_column)
    source_term = jnp.where(struck, coefficient, jnp.float32(0.0))
    previous = field
    current = field
    energy = jnp.zeros(speed.shape, jnp.float32)
    surfaces = []
    for instant in range(STEPS):
        padded = extend(current)
        laplacian = padded[:, 2:, 1:-1, 1:-1] + padded[:, :-2, 1:-1, 1:-1]
        laplacian = laplacian + padded[:, 1:-1, 2:, 1:-1] + padded[:, 1:-1, :-2, 1:-1]
        laplacian = laplacian + padded[:, 1:-1, 1:-1, 2:] + padded[:, 1:-1, 1:-1, :-2]
        laplacian = laplacian - 6.0 * current
        advanced = 2.0 * current - previous + coefficient * laplacian
        advanced = advanced + source_term * (AMPLITUDE * wavelet(instant))
        energy = energy + advanced * advanced
        surfaces.append(advanced[:, 0])
        previous, current = (current, advanced)
    return (energy / STEPS, jnp.stack(surfaces, axis=1))


def by_depth(velocity, initial_field, anchor_x, anchor_y, source_cell, receivers):
    slab_index = lax.axis_index("slab")
    layers, width_x, width_y = velocity.shape
    shot_count = initial_field.shape[0]
    window_rows = initial_field.shape[2]
    window_cols = initial_field.shape[3]

    def cut_window(start_x, start_y):
        return lax.dynamic_slice(
            velocity, (jnp.int32(0), start_x, start_y), (layers, window_rows, window_cols)
        )

    windows = jax.vmap(cut_window)(anchor_x, anchor_y)
    depth_start = slab_index * layers

    def extend_depth(current):
        rimmed = with_halo(current, (("slab", 1),), 1)
        return jnp.pad(rimmed, ((0, 0), (0, 0), (1, 1), (1, 1)))

    energy_here, surface = propagate(windows, initial_field, extend_depth, source_cell, depth_start)
    local_rows = surface.shape[2]
    receiver_row = receivers // window_cols
    receiver_column = receivers % window_cols
    holds = (receiver_row >= 0) & (receiver_row < local_rows) & (depth_start == 0)
    flat_local = jnp.clip(receiver_row, 0, local_rows - 1) * window_cols + receiver_column
    record_count = receivers.shape[1]
    picked = jnp.take_along_axis(
        surface.reshape(shot_count, STEPS, -1),
        jnp.broadcast_to(flat_local[:, None, :], (shot_count, STEPS, record_count)),
        axis=2,
    )
    picked = jnp.where(holds[:, None, :], picked, jnp.float32(0.0))
    traces = lax.psum(picked, "slab")
    partial_image = jnp.zeros((layers, width_x, width_y), jnp.float32)
    corner = (jnp.int32(0), anchor_x[0], anchor_y[0])
    partial_image = lax.dynamic_update_slice(partial_image, energy_here[0], corner)
    summed = lax.psum_scatter(partial_image, "shot", scatter_dimension=1, tiled=True)
    return (traces, summed)


def small_vmem(name, **options):
    return dict(compiler_params=pltpu.CompilerParams(vmem_limit_bytes=VMEM_LIMIT, **options), name=name)


def strip_of(place, slabs):
    return place % 2 * (slabs // 2) + place // 2


def strip_pack(window_rows, window_cols, width_x, slabs, strip, records):
    tall = strip + 2 * STEPS

    def body(anchor_x, anchor_y, receivers, velocity, field, *rest):
        blocks, (facts, listed, speed, pressure, planes, sems) = rest[:slabs], rest[slabs:]
        mine = lax.axis_index("slab")
        top, left = anchor_x[0], anchor_y[0]
        begin = pl.multiple_of(jnp.minimum(top // SUBLANES * SUBLANES, width_x - window_rows - SUBLANES), SUBLANES)
        pltpu.make_async_copy(field.at[0, 0], pressure, sems.at[0]).start()
        for t in range(window_rows // SUBLANES + 1):
            place = window_rows if t == window_rows // SUBLANES else (begin + t * SUBLANES) % window_rows
            pltpu.make_async_copy(
                velocity.at[0, pl.ds(pl.multiple_of(begin + t * SUBLANES, SUBLANES), SUBLANES)],
                speed.at[pl.ds(pl.multiple_of(place, SUBLANES), SUBLANES)],
                sems.at[1],
            ).start()
        listing = pltpu.make_async_copy(receivers, listed, sems.at[2])
        listing.start()
        kinds = lax.broadcasted_iota(jnp.int32, facts.shape, 0)
        facts[...] = jnp.where(kinds == 0, top, left)
        pltpu.make_async_copy(field.at[0, 0], pressure, sems.at[0]).wait()
        rolled = pltpu.roll(pressure[...], left % window_cols, axis=1)
        rolled = pltpu.roll(rolled, (top + STEPS) % window_rows, axis=0)
        planes[0, :window_rows] = rolled
        planes[0, window_rows:] = rolled[: 2 * STEPS]
        pltpu.make_async_copy(velocity.at[0, : window_rows + SUBLANES], speed, sems.at[1]).wait()
        seam = pl.ds(pl.multiple_of(begin % window_rows, SUBLANES), SUBLANES)
        below = lax.broadcasted_iota(jnp.int32, (SUBLANES, 2 * window_cols), 0) < top - begin
        speed[seam] = jnp.where(below, speed[window_rows:], speed[seam])
        columns = lax.broadcasted_iota(jnp.int32, (window_rows, window_cols), 1)
        chosen = COURANT * jnp.where(
            columns >= left, speed[:window_rows, :window_cols], speed[:window_rows, window_cols:]
        )
        coefficient = pltpu.roll(chosen * chosen, STEPS, axis=0)
        planes[1, :window_rows] = coefficient
        planes[1, window_rows:] = coefficient[: 2 * STEPS]
        for k in range(slabs):
            start = pl.multiple_of(strip_of(mine ^ k, slabs) * strip, SUBLANES)
            blocks[k][:tall] = planes[0, pl.ds(start, tall), :]
            blocks[k][tall:] = planes[1, pl.ds(start, tall), :]
        listing.wait()

    hbm = pl.BlockSpec(memory_space=pltpu.HBM)
    smem = pl.BlockSpec(memory_space=pltpu.SMEM)
    vmem = pl.BlockSpec(memory_space=pltpu.VMEM)
    return pl.pallas_call(
        body,
        out_shape=[jax.ShapeDtypeStruct((2 * tall, window_cols), jnp.float32)] * slabs
        + [
            jax.ShapeDtypeStruct((SUBLANES, window_cols), jnp.int32),
            jax.ShapeDtypeStruct((1, records), jnp.int32),
        ],
        in_specs=[smem, smem] + [hbm] * 3,
        out_specs=[vmem] * (slabs + 2),
        scratch_shapes=[
            pltpu.VMEM((window_rows + SUBLANES, 2 * window_cols), jnp.float32),
            pltpu.VMEM((window_rows, window_cols), jnp.float32),
            pltpu.VMEM((2, window_rows + 2 * STEPS, window_cols), jnp.float32),
            pltpu.SemaphoreType.DMA((3,)),
        ],
        **small_vmem("strip_pack"),
    )


def strip_steps(window_rows, window_cols, slabs, strip, records, order, chunks):
    tall = strip + 2 * STEPS
    pieces = window_cols // LANES
    sizes = [len(chunk) * pieces * strip for chunk in chunks]
    heard_rows = records // LANES * STEPS

    def body(source, facts, receivers, *rest):
        blocks, outs = dict(zip(order, rest)), rest[slabs:-4]
        keeps, gives = outs[: len(chunks)], outs[len(chunks) :]
        fields, speeds, energy, surface = rest[-4:]
        mine = lax.axis_index("slab")
        core = lax.axis_index("shot") % 2
        top, left = facts[0:1], facts[1:2]
        for k in range(slabs):
            fields[0, mine ^ k] = blocks[k][:tall]
            speeds[mine ^ k] = blocks[k][tall:]
        rows = lax.broadcasted_iota(jnp.int32, (tall, window_cols), 0)
        columns = lax.broadcasted_iota(jnp.int32, (tall, window_cols), 1)
        begin = strip_of(mine, slabs) * strip - STEPS

        def local_row(row):
            return (row + top - begin + window_rows) % window_rows

        def local_column(column):
            return (column + left) % window_cols

        inside_up = rows != local_row(0)
        inside_down = rows != local_row(window_rows - 1)
        inside_left = columns != local_column(0)
        inside_right = columns != local_column(window_cols - 1)
        struck = (rows == local_row(source[0] // window_cols)) & (columns == local_column(source[0] % window_cols))
        source_term = jnp.where(struck, speeds[1], 0.0)
        for instant in range(STEPS):
            now, then = instant % 2, (instant + 1) % 2
            for level in range(slabs):
                current = fields[now, level]
                previous = fields[then if instant else now, level]
                laplacian = jnp.where(inside_up, pltpu.roll(current, 1, axis=0), 0.0)
                laplacian = laplacian + jnp.where(inside_down, pltpu.roll(current, tall - 1, axis=0), 0.0)
                laplacian = laplacian + jnp.where(inside_left, pltpu.roll(current, 1, axis=1), 0.0)
                laplacian = laplacian + jnp.where(inside_right, pltpu.roll(current, window_cols - 1, axis=1), 0.0)
                if level > 0:
                    laplacian = laplacian + fields[now, level - 1]
                if level < slabs - 1:
                    laplacian = laplacian + fields[now, level + 1]
                laplacian = laplacian - 6.0 * current
                advanced = 2.0 * current - previous + speeds[level] * laplacian
                if level == 1:
                    advanced = advanced + source_term * (AMPLITUDE * wavelet(instant))
                if level == 0:
                    surface[instant * tall : (instant + 1) * tall] = advanced
                if instant < STEPS - 1:
                    fields[then, level] = advanced
                square = advanced * advanced
                energy[level] = square if instant == 0 else energy[level] + square
        for parts, parity in ((gives, 1 - core), (keeps, core)):
            for out, chunk, size in zip(parts, chunks, sizes):
                for j, k in enumerate(chunk):
                    level = 2 * ((mine // 2) ^ k) + parity
                    for i in range(pieces):
                        at = (j * pieces + i) * strip
                        cells = energy[level, STEPS : STEPS + strip, i * LANES : (i + 1) * LANES]
                        out[at : at + strip] = cells / STEPS
                out[size : size + SUBLANES] = facts[:, :LANES].astype(jnp.float32)
        row = (receivers[...] // window_cols + top[:, :1]) % window_rows - begin
        column = (receivers[...] % window_cols + left[:, :1]) % window_cols
        row = jnp.where((row >= STEPS) & (row < STEPS + strip), row, -1)
        cells = lax.broadcasted_iota(jnp.int32, (window_cols, records), 0)
        chosen = jnp.where(cells == column, 1.0, 0.0)
        picked = jnp.dot(surface[...], chosen, precision=lax.Precision.HIGHEST, preferred_element_type=jnp.float32)
        places = lax.broadcasted_iota(jnp.int32, (tall, records), 0)
        for n in range(STEPS):
            own = jnp.where(places == row, picked[n * tall : (n + 1) * tall], 0.0)
            own = jnp.sum(own, axis=0, keepdims=True)
            for i in range(records // LANES):
                at = sizes[0] + SUBLANES + i * STEPS + n
                for out in (keeps[0], gives[0]):
                    out[at : at + 1] = own[:, i * LANES : (i + 1) * LANES]

    vmem = pl.BlockSpec(memory_space=pltpu.VMEM)
    return pl.pallas_call(
        body,
        out_shape=[
            jax.ShapeDtypeStruct((size + SUBLANES + (0 if c else heard_rows), LANES), jnp.float32)
            for c, size in enumerate(sizes)
        ]
        * 2,
        in_specs=[pl.BlockSpec(memory_space=pltpu.SMEM)] + [vmem] * (2 + slabs),
        out_specs=[vmem] * (2 * len(chunks)),
        scratch_shapes=[
            pltpu.VMEM((2, slabs, tall, window_cols), jnp.float32),
            pltpu.VMEM((slabs, tall, window_cols), jnp.float32),
            pltpu.VMEM((slabs, tall, window_cols), jnp.float32),
            pltpu.VMEM((STEPS * tall, window_cols), jnp.float32),
        ],
        **small_vmem("strip_steps"),
    )


def strip_share(window_rows, window_cols, width_y, rows_here, strip, records, count, tells):
    pieces = window_cols // LANES
    wide = width_y // LANES
    deep = count * pieces * strip
    heard_rows = records // LANES * STEPS

    def body(keep, got, *outs):
        mine, shot = lax.axis_index("slab"), lax.axis_index("shot")
        zone, side = mine // 2, mine % 2
        shares = (keep, got)
        tags = [share[deep : deep + SUBLANES].astype(jnp.int32) for share in shares]
        columns = lax.broadcasted_iota(jnp.int32, (strip, LANES), 1)
        for out, over_x in zip(outs, (1, 0)):
            to_shot = ((shot // 2) ^ over_x) * 2 + side
            rows = lax.broadcasted_iota(jnp.int32, (strip, LANES), 0) + to_shot * rows_here + zone * strip
            insides = []
            for tag in tags:
                down, along = rows - tag[0:1], columns - tag[1:2]
                tall = (down >= 0) & (down < window_rows)
                insides.append(
                    [tall & (along >= -i * LANES) & (along < window_cols - i * LANES) for i in range(wide)]
                )
            for j in range(count):
                for i in range(wide):
                    start = (j * pieces + i % pieces) * strip
                    parts = [
                        jnp.where(inside[i], share[start : start + strip], 0.0)
                        for share, inside in zip(shares, insides)
                    ]
                    at = (j * wide + i) * strip
                    out[at : at + strip] = parts[0] + parts[1]
        if tells:
            heard, told = outs[2:]
            same_core = shot % 2 == side
            heard[...] = jnp.where(same_core, keep[deep + SUBLANES :], got[deep + SUBLANES :])
            told[...] = jnp.where(same_core, got[deep + SUBLANES :], keep[deep + SUBLANES :])

    vmem = pl.BlockSpec(memory_space=pltpu.VMEM)
    sizes = [count * wide * strip] * 2 + [heard_rows] * (2 * tells)
    return pl.pallas_call(
        body,
        out_shape=[jax.ShapeDtypeStruct((size, LANES), jnp.float32) for size in sizes],
        in_specs=[vmem] * 2,
        out_specs=[vmem] * len(sizes),
        **small_vmem("strip_share"),
    )


def strip_sum(width_y, strip, records, count):
    deep = width_y // LANES * strip
    heard_rows = records // LANES * STEPS

    def body(come, own, heard_too, heard, *outs):
        for j, out in enumerate(outs):
            out[:deep] = own[j * deep : (j + 1) * deep] + come[j * deep : (j + 1) * deep]
            out[deep:] = heard[...] + heard_too[...]

    vmem = pl.BlockSpec(memory_space=pltpu.VMEM)
    return pl.pallas_call(
        body,
        out_shape=[jax.ShapeDtypeStruct((deep + heard_rows, LANES), jnp.float32)] * count,
        in_specs=[vmem] * 4,
        out_specs=[vmem] * count,
        **small_vmem("strip_sum"),
    )


def strip_place(width_y, rows_here, slabs, strip, records, order):
    wide = width_y // LANES
    pairs = slabs // 2

    def body(*rest):
        blocks, (traces, image) = dict(zip(order, rest)), rest[pairs:]
        zone = lax.axis_index("slab") // 2
        for k in range(pairs):
            start = pl.multiple_of((zone ^ k) * strip, SUBLANES)
            for i in range(wide):
                image[0, pl.ds(start, strip), i * LANES : (i + 1) * LANES] = blocks[k][i * strip : (i + 1) * strip]
        total = blocks[0][wide * strip :]
        for k in range(1, pairs):
            total = total + blocks[k][wide * strip :]
        for i in range(records // LANES):
            traces[0, :, i * LANES : (i + 1) * LANES] = total[i * STEPS : (i + 1) * STEPS]

    vmem = pl.BlockSpec(memory_space=pltpu.VMEM)
    return pl.pallas_call(
        body,
        out_shape=[
            jax.ShapeDtypeStruct((1, STEPS, records), jnp.float32),
            jax.ShapeDtypeStruct((1, rows_here, width_y), jnp.float32),
        ],
        in_specs=[vmem] * pairs,
        out_specs=[vmem] * 2,
        **small_vmem("strip_place"),
    )


def swap(array, axis, k):
    return lax.ppermute(array, axis, [(i, i ^ k) for i in range(lax.axis_size(axis))])


def far_first(count):
    return list(reversed(range(count)))


def cross(array, k):
    slabs, shots = lax.axis_size("slab"), lax.axis_size("shot")
    pairs = []
    for place in range(slabs):
        for shot in range(shots):
            side, core = place % 2, shot % 2
            to_place = ((place // 2) ^ k) * 2 + core
            to_shot = shot // 2 * 2 + side
            pairs.append((place * shots + shot, to_place * shots + to_shot))
    return lax.ppermute(array, ("slab", "shot"), pairs)


def by_strips(velocity, initial_field, anchor_x, anchor_y, source_cell, receivers):
    slabs, shots = lax.axis_size("slab"), lax.axis_size("shot")
    window_rows, window_cols = initial_field.shape[2:]
    width_y = velocity.shape[2]
    rows_here = velocity.shape[1] // shots
    strip = window_rows // slabs
    records = receivers.shape[1]
    velocity, initial_field, receivers = (
        pltpu.with_memory_space_constraint(array, pltpu.HBM) for array in (velocity, initial_field, receivers)
    )
    *packed, facts, listed = strip_pack(window_rows, window_cols, velocity.shape[1], slabs, strip, records)(
        anchor_x, anchor_y, receivers, velocity, initial_field
    )
    order = far_first(slabs)
    held = [swap(packed[k], "slab", k) if k else packed[k] for k in order]
    pairs = slabs // 2
    chunks = ((*range(pairs // 2, pairs),), (*range(pairs // 2 - 1, -1, -1),))
    zones = [k for chunk in chunks for k in chunk]
    outs = strip_steps(window_rows, window_cols, slabs, strip, records, order, chunks)(
        source_cell, facts, listed, *held
    )
    keeps, gives = outs[: len(chunks)], outs[len(chunks) :]
    gots = []
    for give in gives:
        gots.append(swap(give, "shot", 1))
    shares, notes = [], []
    for c, chunk in enumerate(chunks):
        leave, stay, *more = strip_share(
            window_rows, window_cols, width_y, rows_here, strip, records, len(chunk), c == 0
        )(keeps[c], gots[c])
        shares.append((swap(leave, "shot", 2), stay))
        notes += more
    heard, told = notes
    heard_too = swap(told, "slab", 1)
    back = []
    for chunk, (come, stay) in zip(chunks, shares):
        sums = strip_sum(width_y, strip, records, len(chunk))(come, stay, heard_too, heard)
        for part, k in zip(sums, chunk):
            back.append(cross(part, k))
    traces, image = strip_place(width_y, rows_here, slabs, strip, records, zones)(*back)
    return (traces, image)


def strips_fit(mesh, velocity, initial_field, receivers):
    slabs, shots = mesh.shape["slab"], mesh.shape["shot"]
    layers, width_x, width_y = velocity.shape
    shot_count, levels, window_rows, window_cols = initial_field.shape
    records = receivers.shape[1]
    return (
        layers == levels == slabs
        and slabs == 8
        and shot_count == shots == 4
        and width_x == 2 * window_rows
        and width_y == 2 * window_cols
        and window_rows % (slabs * SUBLANES) == 0
        and width_x // shots == window_rows // 2
        and window_rows // slabs + 2 * STEPS <= window_rows
        and window_cols % LANES == 0
        and records % (2 * LANES) == 0
        and (2 * STEPS) % SUBLANES == 0
    )


def solution(mesh):
    placed = (
        P("slab", None, None),
        P("shot", "slab", None, None),
        P("shot"),
        P("shot"),
        P("shot"),
        P("shot", None),
    )

    def whole(velocity, initial_field, anchor_x, anchor_y, source_cell, receivers):
        fit = strips_fit(mesh, velocity, initial_field, receivers)
        step = jax.shard_map(
            by_strips if fit else by_depth,
            mesh=mesh,
            in_specs=placed,
            out_specs=(P("shot", None, None), P("slab", "shot", None)),
            check_vma=False,
        )
        return step(velocity, initial_field, anchor_x, anchor_y, source_cell, receivers)

    return whole
```

```python
import math

import jax
import jax.numpy as jnp
from jax import lax
from jax.experimental import pallas as pl
from jax.experimental.pallas import tpu as pltpu
from jax.sharding import PartitionSpec as P


STEPS = 4


COURANT = 0.125
AMPLITUDE = 4.0

SUBLANES = 8
LANES = 128
VMEM_LIMIT = 16 * 1024 * 1024


def wavelet(instant):
    shifted = 0.8 * (instant - 1.5)
    return (1.0 - 2.0 * shifted * shifted) * math.exp(-shifted * shifted)


def with_halo(cells, sides, width):
    for axis, dim in sides:
        count = lax.axis_size(axis)
        ends = count - 1
        head = lax.slice_in_dim(cells, 0, width, axis=dim)
        tail = lax.slice_in_dim(cells, cells.shape[dim] - width, cells.shape[dim], axis=dim)
        cells = jnp.concatenate(
            [
                lax.ppermute(tail, axis, [(i, (i + 1) % count) for i in range(ends)]),
                cells,
                lax.ppermute(head, axis, [((i + 1) % count, i) for i in range(ends)]),
            ],
            axis=dim,
        )
    return cells


def propagate(speed, field, extend, source, depth_start):
    coefficient = jnp.square(COURANT * speed)
    column_count = speed.shape[3]
    depth_place = lax.broadcasted_iota(jnp.int32, speed.shape, 1) + depth_start
    row_place = lax.broadcasted_iota(jnp.int32, speed.shape, 2)
    column_place = lax.broadcasted_iota(jnp.int32, speed.shape, 3)
    source_row = (source // column_count)[:, None, None, None]
    source_column = (source % column_count)[:, None, None, None]
    struck = (depth_place == 1) & (row_place == source_row) & (column_place == source_column)
    source_term = jnp.where(struck, coefficient, jnp.float32(0.0))
    previous = field
    current = field
    energy = jnp.zeros(speed.shape, jnp.float32)
    surfaces = []
    for instant in range(STEPS):
        padded = extend(current)
        laplacian = padded[:, 2:, 1:-1, 1:-1] + padded[:, :-2, 1:-1, 1:-1]
        laplacian = laplacian + padded[:, 1:-1, 2:, 1:-1] + padded[:, 1:-1, :-2, 1:-1]
        laplacian = laplacian + padded[:, 1:-1, 1:-1, 2:] + padded[:, 1:-1, 1:-1, :-2]
        laplacian = laplacian - 6.0 * current
        advanced = 2.0 * current - previous + coefficient * laplacian
        advanced = advanced + source_term * (AMPLITUDE * wavelet(instant))
        energy = energy + advanced * advanced
        surfaces.append(advanced[:, 0])
        previous, current = (current, advanced)
    return (energy / STEPS, jnp.stack(surfaces, axis=1))


def by_depth(velocity, initial_field, anchor_x, anchor_y, source_cell, receivers):
    slab_index = lax.axis_index("slab")
    layers, width_x, width_y = velocity.shape
    shot_count = initial_field.shape[0]
    window_rows = initial_field.shape[2]
    window_cols = initial_field.shape[3]

    def cut_window(start_x, start_y):
        return lax.dynamic_slice(
            velocity, (jnp.int32(0), start_x, start_y), (layers, window_rows, window_cols)
        )

    windows = jax.vmap(cut_window)(anchor_x, anchor_y)
    depth_start = slab_index * layers

    def extend_depth(current):
        rimmed = with_halo(current, (("slab", 1),), 1)
        return jnp.pad(rimmed, ((0, 0), (0, 0), (1, 1), (1, 1)))

    energy_here, surface = propagate(windows, initial_field, extend_depth, source_cell, depth_start)
    local_rows = surface.shape[2]
    receiver_row = receivers // window_cols
    receiver_column = receivers % window_cols
    holds = (receiver_row >= 0) & (receiver_row < local_rows) & (depth_start == 0)
    flat_local = jnp.clip(receiver_row, 0, local_rows - 1) * window_cols + receiver_column
    record_count = receivers.shape[1]
    picked = jnp.take_along_axis(
        surface.reshape(shot_count, STEPS, -1),
        jnp.broadcast_to(flat_local[:, None, :], (shot_count, STEPS, record_count)),
        axis=2,
    )
    picked = jnp.where(holds[:, None, :], picked, jnp.float32(0.0))
    traces = lax.psum(picked, "slab")
    partial_image = jnp.zeros((layers, width_x, width_y), jnp.float32)
    corner = (jnp.int32(0), anchor_x[0], anchor_y[0])
    partial_image = lax.dynamic_update_slice(partial_image, energy_here[0], corner)
    summed = lax.psum_scatter(partial_image, "shot", scatter_dimension=1, tiled=True)
    return (traces, summed)


def small_vmem(name, **options):
    return dict(compiler_params=pltpu.CompilerParams(vmem_limit_bytes=VMEM_LIMIT, **options), name=name)


def strip_of(place, slabs):
    return place % 2 * (slabs // 2) + place // 2


def strip_pack(window_rows, window_cols, width_x, slabs, strip, records):
    tall = strip + 2 * STEPS

    def body(anchor_x, anchor_y, receivers, velocity, field, *rest):
        blocks, (facts, listed, speed, pressure, planes, sems) = rest[:slabs], rest[slabs:]
        mine = lax.axis_index("slab")
        top, left = anchor_x[0], anchor_y[0]
        begin = pl.multiple_of(jnp.minimum(top // SUBLANES * SUBLANES, width_x - window_rows - SUBLANES), SUBLANES)
        pltpu.make_async_copy(field.at[0, 0], pressure, sems.at[0]).start()
        for t in range(window_rows // SUBLANES + 1):
            place = window_rows if t == window_rows // SUBLANES else (begin + t * SUBLANES) % window_rows
            pltpu.make_async_copy(
                velocity.at[0, pl.ds(pl.multiple_of(begin + t * SUBLANES, SUBLANES), SUBLANES)],
                speed.at[pl.ds(pl.multiple_of(place, SUBLANES), SUBLANES)],
                sems.at[1],
            ).start()
        listing = pltpu.make_async_copy(receivers, listed, sems.at[2])
        listing.start()
        kinds = lax.broadcasted_iota(jnp.int32, facts.shape, 0)
        facts[...] = jnp.where(kinds == 0, top, left)
        pltpu.make_async_copy(field.at[0, 0], pressure, sems.at[0]).wait()
        rolled = pltpu.roll(pressure[...], left % window_cols, axis=1)
        rolled = pltpu.roll(rolled, (top + STEPS) % window_rows, axis=0)
        planes[0, :window_rows] = rolled
        planes[0, window_rows:] = rolled[: 2 * STEPS]
        pltpu.make_async_copy(velocity.at[0, : window_rows + SUBLANES], speed, sems.at[1]).wait()
        seam = pl.ds(pl.multiple_of(begin % window_rows, SUBLANES), SUBLANES)
        below = lax.broadcasted_iota(jnp.int32, (SUBLANES, 2 * window_cols), 0) < top - begin
        speed[seam] = jnp.where(below, speed[window_rows:], speed[seam])
        columns = lax.broadcasted_iota(jnp.int32, (window_rows, window_cols), 1)
        chosen = COURANT * jnp.where(
            columns >= left, speed[:window_rows, :window_cols], speed[:window_rows, window_cols:]
        )
        coefficient = pltpu.roll(chosen * chosen, STEPS, axis=0)
        planes[1, :window_rows] = coefficient
        planes[1, window_rows:] = coefficient[: 2 * STEPS]
        for k in range(slabs):
            start = pl.multiple_of(strip_of(mine ^ k, slabs) * strip, SUBLANES)
            blocks[k][:tall] = planes[0, pl.ds(start, tall), :]
            blocks[k][tall:] = planes[1, pl.ds(start, tall), :]
        listing.wait()

    hbm = pl.BlockSpec(memory_space=pltpu.HBM)
    smem = pl.BlockSpec(memory_space=pltpu.SMEM)
    vmem = pl.BlockSpec(memory_space=pltpu.VMEM)
    return pl.pallas_call(
        body,
        out_shape=[jax.ShapeDtypeStruct((2 * tall, window_cols), jnp.float32)] * slabs
        + [
            jax.ShapeDtypeStruct((SUBLANES, window_cols), jnp.int32),
            jax.ShapeDtypeStruct((1, records), jnp.int32),
        ],
        in_specs=[smem, smem] + [hbm] * 3,
        out_specs=[vmem] * (slabs + 2),
        scratch_shapes=[
            pltpu.VMEM((window_rows + SUBLANES, 2 * window_cols), jnp.float32),
            pltpu.VMEM((window_rows, window_cols), jnp.float32),
            pltpu.VMEM((2, window_rows + 2 * STEPS, window_cols), jnp.float32),
            pltpu.SemaphoreType.DMA((3,)),
        ],
        **small_vmem("strip_pack"),
    )


def strip_steps(window_rows, window_cols, slabs, strip, records, order, chunks):
    tall = strip + 2 * STEPS
    pieces = window_cols // LANES
    sizes = [len(chunk) * pieces * strip for chunk in chunks]
    heard_rows = records // LANES * STEPS

    def body(source, facts, receivers, *rest):
        blocks, outs = dict(zip(order, rest)), rest[slabs:-4]
        keeps, gives = outs[: len(chunks)], outs[len(chunks) :]
        fields, speeds, energy, surface = rest[-4:]
        mine = lax.axis_index("slab")
        core = lax.axis_index("shot") % 2
        top, left = facts[0:1], facts[1:2]
        for k in range(slabs):
            fields[0, mine ^ k] = blocks[k][:tall]
            speeds[mine ^ k] = blocks[k][tall:]
        rows = lax.broadcasted_iota(jnp.int32, (tall, window_cols), 0)
        columns = lax.broadcasted_iota(jnp.int32, (tall, window_cols), 1)
        begin = strip_of(mine, slabs) * strip - STEPS

        def local_row(row):
            return (row + top - begin + window_rows) % window_rows

        def local_column(column):
            return (column + left) % window_cols

        inside_up = jnp.where(rows != local_row(0), 1.0, 0.0)
        inside_down = jnp.where(rows != local_row(window_rows - 1), 1.0, 0.0)
        inside_left = jnp.where(columns != local_column(0), 1.0, 0.0)
        inside_right = jnp.where(columns != local_column(window_cols - 1), 1.0, 0.0)
        struck = (rows == local_row(source[0] // window_cols)) & (columns == local_column(source[0] % window_cols))
        source_term = jnp.where(struck, speeds[1], 0.0)
        for instant in range(STEPS):
            now, then = instant % 2, (instant + 1) % 2
            for level in range(slabs):
                current = fields[now, level]
                previous = fields[then if instant else now, level]
                laplacian = inside_up * pltpu.roll(current, 1, axis=0)
                laplacian = laplacian + inside_down * pltpu.roll(current, tall - 1, axis=0)
                laplacian = laplacian + inside_left * pltpu.roll(current, 1, axis=1)
                laplacian = laplacian + inside_right * pltpu.roll(current, window_cols - 1, axis=1)
                if level > 0:
                    laplacian = laplacian + fields[now, level - 1]
                if level < slabs - 1:
                    laplacian = laplacian + fields[now, level + 1]
                laplacian = laplacian - 6.0 * current
                advanced = 2.0 * current - previous + speeds[level] * laplacian
                if level == 1:
                    advanced = advanced + source_term * (AMPLITUDE * wavelet(instant))
                if level == 0:
                    surface[instant * tall : (instant + 1) * tall] = advanced
                if instant < STEPS - 1:
                    fields[then, level] = advanced
                square = advanced * advanced
                energy[level] = square if instant == 0 else energy[level] + square
        for parts, parity in ((gives, 1 - core), (keeps, core)):
            for out, chunk, size in zip(parts, chunks, sizes):
                for j, k in enumerate(chunk):
                    level = 2 * ((mine // 2) ^ k) + parity
                    for i in range(pieces):
                        at = (j * pieces + i) * strip
                        cells = energy[level, STEPS : STEPS + strip, i * LANES : (i + 1) * LANES]
                        out[at : at + strip] = cells / STEPS
                out[size : size + SUBLANES] = facts[:, :LANES].astype(jnp.float32)
        row = (receivers[...] // window_cols + top[:, :1]) % window_rows - begin
        column = (receivers[...] % window_cols + left[:, :1]) % window_cols
        row = jnp.where((row >= STEPS) & (row < STEPS + strip), row, -1)
        cells = lax.broadcasted_iota(jnp.int32, (window_cols, records), 0)
        chosen = jnp.where(cells == column, 1.0, 0.0)
        picked = jnp.dot(surface[...], chosen, precision=lax.Precision.HIGHEST, preferred_element_type=jnp.float32)
        places = lax.broadcasted_iota(jnp.int32, (tall, records), 0)
        for n in range(STEPS):
            own = jnp.where(places == row, picked[n * tall : (n + 1) * tall], 0.0)
            own = jnp.sum(own, axis=0, keepdims=True)
            for i in range(records // LANES):
                at = sizes[0] + SUBLANES + i * STEPS + n
                for out in (keeps[0], gives[0]):
                    out[at : at + 1] = own[:, i * LANES : (i + 1) * LANES]

    vmem = pl.BlockSpec(memory_space=pltpu.VMEM)
    return pl.pallas_call(
        body,
        out_shape=[
            jax.ShapeDtypeStruct((size + SUBLANES + (0 if c else heard_rows), LANES), jnp.float32)
            for c, size in enumerate(sizes)
        ]
        * 2,
        in_specs=[pl.BlockSpec(memory_space=pltpu.SMEM)] + [vmem] * (2 + slabs),
        out_specs=[vmem] * (2 * len(chunks)),
        scratch_shapes=[
            pltpu.VMEM((2, slabs, tall, window_cols), jnp.float32),
            pltpu.VMEM((slabs, tall, window_cols), jnp.float32),
            pltpu.VMEM((slabs, tall, window_cols), jnp.float32),
            pltpu.VMEM((STEPS * tall, window_cols), jnp.float32),
        ],
        **small_vmem("strip_steps"),
    )


def strip_share(window_rows, window_cols, width_y, rows_here, strip, records, count, tells):
    pieces = window_cols // LANES
    wide = width_y // LANES
    deep = count * pieces * strip
    heard_rows = records // LANES * STEPS

    def body(keep, got, *outs):
        mine, shot = lax.axis_index("slab"), lax.axis_index("shot")
        zone, side = mine // 2, mine % 2
        shares = (keep, got)
        tags = [share[deep : deep + SUBLANES].astype(jnp.int32) for share in shares]
        columns = lax.broadcasted_iota(jnp.int32, (strip, LANES), 1)
        for out, over_x in zip(outs, (1, 0)):
            to_shot = ((shot // 2) ^ over_x) * 2 + side
            rows = lax.broadcasted_iota(jnp.int32, (strip, LANES), 0) + to_shot * rows_here + zone * strip
            insides = []
            for tag in tags:
                down, along = rows - tag[0:1], columns - tag[1:2]
                tall = (down >= 0) & (down < window_rows)
                insides.append(
                    [tall & (along >= -i * LANES) & (along < window_cols - i * LANES) for i in range(wide)]
                )
            for j in range(count):
                for i in range(wide):
                    start = (j * pieces + i % pieces) * strip
                    parts = [
                        jnp.where(inside[i], share[start : start + strip], 0.0)
                        for share, inside in zip(shares, insides)
                    ]
                    at = (j * wide + i) * strip
                    out[at : at + strip] = parts[0] + parts[1]
        if tells:
            heard, told = outs[2:]
            same_core = shot % 2 == side
            heard[...] = jnp.where(same_core, keep[deep + SUBLANES :], got[deep + SUBLANES :])
            told[...] = jnp.where(same_core, got[deep + SUBLANES :], keep[deep + SUBLANES :])

    vmem = pl.BlockSpec(memory_space=pltpu.VMEM)
    sizes = [count * wide * strip] * 2 + [heard_rows] * (2 * tells)
    return pl.pallas_call(
        body,
        out_shape=[jax.ShapeDtypeStruct((size, LANES), jnp.float32) for size in sizes],
        in_specs=[vmem] * 2,
        out_specs=[vmem] * len(sizes),
        **small_vmem("strip_share"),
    )


def strip_sum(width_y, strip, records, count):
    deep = width_y // LANES * strip
    heard_rows = records // LANES * STEPS

    def body(come, own, heard_too, heard, *outs):
        for j, out in enumerate(outs):
            out[:deep] = own[j * deep : (j + 1) * deep] + come[j * deep : (j + 1) * deep]
            out[deep:] = heard[...] + heard_too[...]

    vmem = pl.BlockSpec(memory_space=pltpu.VMEM)
    return pl.pallas_call(
        body,
        out_shape=[jax.ShapeDtypeStruct((deep + heard_rows, LANES), jnp.float32)] * count,
        in_specs=[vmem] * 4,
        out_specs=[vmem] * count,
        **small_vmem("strip_sum"),
    )


def strip_place(width_y, rows_here, slabs, strip, records, order):
    wide = width_y // LANES
    pairs = slabs // 2

    def body(*rest):
        blocks, (traces, image) = dict(zip(order, rest)), rest[pairs:]
        zone = lax.axis_index("slab") // 2
        for k in range(pairs):
            start = pl.multiple_of((zone ^ k) * strip, SUBLANES)
            for i in range(wide):
                image[0, pl.ds(start, strip), i * LANES : (i + 1) * LANES] = blocks[k][i * strip : (i + 1) * strip]
        total = blocks[0][wide * strip :]
        for k in range(1, pairs):
            total = total + blocks[k][wide * strip :]
        for i in range(records // LANES):
            traces[0, :, i * LANES : (i + 1) * LANES] = total[i * STEPS : (i + 1) * STEPS]

    vmem = pl.BlockSpec(memory_space=pltpu.VMEM)
    return pl.pallas_call(
        body,
        out_shape=[
            jax.ShapeDtypeStruct((1, STEPS, records), jnp.float32),
            jax.ShapeDtypeStruct((1, rows_here, width_y), jnp.float32),
        ],
        in_specs=[vmem] * pairs,
        out_specs=[vmem] * 2,
        **small_vmem("strip_place"),
    )


def swap(array, axis, k):
    return lax.ppermute(array, axis, [(i, i ^ k) for i in range(lax.axis_size(axis))])


def far_first(count):
    return list(reversed(range(count)))


def cross(array, k):
    slabs, shots = lax.axis_size("slab"), lax.axis_size("shot")
    pairs = []
    for place in range(slabs):
        for shot in range(shots):
            side, core = place % 2, shot % 2
            to_place = ((place // 2) ^ k) * 2 + core
            to_shot = shot // 2 * 2 + side
            pairs.append((place * shots + shot, to_place * shots + to_shot))
    return lax.ppermute(array, ("slab", "shot"), pairs)


def by_strips(velocity, initial_field, anchor_x, anchor_y, source_cell, receivers):
    slabs, shots = lax.axis_size("slab"), lax.axis_size("shot")
    window_rows, window_cols = initial_field.shape[2:]
    width_y = velocity.shape[2]
    rows_here = velocity.shape[1] // shots
    strip = window_rows // slabs
    records = receivers.shape[1]
    velocity, initial_field, receivers = (
        pltpu.with_memory_space_constraint(array, pltpu.HBM) for array in (velocity, initial_field, receivers)
    )
    *packed, facts, listed = strip_pack(window_rows, window_cols, velocity.shape[1], slabs, strip, records)(
        anchor_x, anchor_y, receivers, velocity, initial_field
    )
    order = far_first(slabs)
    held = [swap(packed[k], "slab", k) if k else packed[k] for k in order]
    pairs = slabs // 2
    chunks = ((*range(pairs // 2, pairs),), (*range(pairs // 2 - 1, -1, -1),))
    zones = [k for chunk in chunks for k in chunk]
    outs = strip_steps(window_rows, window_cols, slabs, strip, records, order, chunks)(
        source_cell, facts, listed, *held
    )
    keeps, gives = outs[: len(chunks)], outs[len(chunks) :]
    gots = []
    for give in gives:
        gots.append(swap(give, "shot", 1))
    shares, notes = [], []
    for c, chunk in enumerate(chunks):
        leave, stay, *more = strip_share(
            window_rows, window_cols, width_y, rows_here, strip, records, len(chunk), c == 0
        )(keeps[c], gots[c])
        shares.append((swap(leave, "shot", 2), stay))
        notes += more
    heard, told = notes
    heard_too = swap(told, "slab", 1)
    back = []
    for chunk, (come, stay) in zip(chunks, shares):
        sums = strip_sum(width_y, strip, records, len(chunk))(come, stay, heard_too, heard)
        for part, k in zip(sums, chunk):
            back.append(cross(part, k))
    traces, image = strip_place(width_y, rows_here, slabs, strip, records, zones)(*back)
    return (traces, image)


def strips_fit(mesh, velocity, initial_field, receivers):
    slabs, shots = mesh.shape["slab"], mesh.shape["shot"]
    layers, width_x, width_y = velocity.shape
    shot_count, levels, window_rows, window_cols = initial_field.shape
    records = receivers.shape[1]
    return (
        layers == levels == slabs
        and slabs == 8
        and shot_count == shots == 4
        and width_x == 2 * window_rows
        and width_y == 2 * window_cols
        and window_rows % (slabs * SUBLANES) == 0
        and width_x // shots == window_rows // 2
        and window_rows // slabs + 2 * STEPS <= window_rows
        and window_cols % LANES == 0
        and records % (2 * LANES) == 0
        and (2 * STEPS) % SUBLANES == 0
    )


def solution(mesh):
    placed = (
        P("slab", None, None),
        P("shot", "slab", None, None),
        P("shot"),
        P("shot"),
        P("shot"),
        P("shot", None),
    )

    def whole(velocity, initial_field, anchor_x, anchor_y, source_cell, receivers):
        fit = strips_fit(mesh, velocity, initial_field, receivers)
        step = jax.shard_map(
            by_strips if fit else by_depth,
            mesh=mesh,
            in_specs=placed,
            out_specs=(P("shot", None, None), P("slab", "shot", None)),
            check_vma=False,
        )
        return step(velocity, initial_field, anchor_x, anchor_y, source_cell, receivers)

    return whole
```

```python
import math

import jax
import jax.numpy as jnp
from jax import lax
from jax.experimental import pallas as pl
from jax.experimental.pallas import tpu as pltpu
from jax.sharding import PartitionSpec as P


STEPS = 4


COURANT = 0.125
AMPLITUDE = 4.0

SUBLANES = 8
LANES = 128
VMEM_LIMIT = 16 * 1024 * 1024


def wavelet(instant):
    shifted = 0.8 * (instant - 1.5)
    return (1.0 - 2.0 * shifted * shifted) * math.exp(-shifted * shifted)


def with_halo(cells, sides, width):
    for axis, dim in sides:
        count = lax.axis_size(axis)
        ends = count - 1
        head = lax.slice_in_dim(cells, 0, width, axis=dim)
        tail = lax.slice_in_dim(cells, cells.shape[dim] - width, cells.shape[dim], axis=dim)
        cells = jnp.concatenate(
            [
                lax.ppermute(tail, axis, [(i, (i + 1) % count) for i in range(ends)]),
                cells,
                lax.ppermute(head, axis, [((i + 1) % count, i) for i in range(ends)]),
            ],
            axis=dim,
        )
    return cells


def propagate(speed, field, extend, source, depth_start):
    coefficient = jnp.square(COURANT * speed)
    column_count = speed.shape[3]
    depth_place = lax.broadcasted_iota(jnp.int32, speed.shape, 1) + depth_start
    row_place = lax.broadcasted_iota(jnp.int32, speed.shape, 2)
    column_place = lax.broadcasted_iota(jnp.int32, speed.shape, 3)
    source_row = (source // column_count)[:, None, None, None]
    source_column = (source % column_count)[:, None, None, None]
    struck = (depth_place == 1) & (row_place == source_row) & (column_place == source_column)
    source_term = jnp.where(struck, coefficient, jnp.float32(0.0))
    previous = field
    current = field
    energy = jnp.zeros(speed.shape, jnp.float32)
    surfaces = []
    for instant in range(STEPS):
        padded = extend(current)
        laplacian = padded[:, 2:, 1:-1, 1:-1] + padded[:, :-2, 1:-1, 1:-1]
        laplacian = laplacian + padded[:, 1:-1, 2:, 1:-1] + padded[:, 1:-1, :-2, 1:-1]
        laplacian = laplacian + padded[:, 1:-1, 1:-1, 2:] + padded[:, 1:-1, 1:-1, :-2]
        laplacian = laplacian - 6.0 * current
        advanced = 2.0 * current - previous + coefficient * laplacian
        advanced = advanced + source_term * (AMPLITUDE * wavelet(instant))
        energy = energy + advanced * advanced
        surfaces.append(advanced[:, 0])
        previous, current = (current, advanced)
    return (energy / STEPS, jnp.stack(surfaces, axis=1))


def by_depth(velocity, initial_field, anchor_x, anchor_y, source_cell, receivers):
    slab_index = lax.axis_index("slab")
    layers, width_x, width_y = velocity.shape
    shot_count = initial_field.shape[0]
    window_rows = initial_field.shape[2]
    window_cols = initial_field.shape[3]

    def cut_window(start_x, start_y):
        return lax.dynamic_slice(
            velocity, (jnp.int32(0), start_x, start_y), (layers, window_rows, window_cols)
        )

    windows = jax.vmap(cut_window)(anchor_x, anchor_y)
    depth_start = slab_index * layers

    def extend_depth(current):
        rimmed = with_halo(current, (("slab", 1),), 1)
        return jnp.pad(rimmed, ((0, 0), (0, 0), (1, 1), (1, 1)))

    energy_here, surface = propagate(windows, initial_field, extend_depth, source_cell, depth_start)
    local_rows = surface.shape[2]
    receiver_row = receivers // window_cols
    receiver_column = receivers % window_cols
    holds = (receiver_row >= 0) & (receiver_row < local_rows) & (depth_start == 0)
    flat_local = jnp.clip(receiver_row, 0, local_rows - 1) * window_cols + receiver_column
    record_count = receivers.shape[1]
    picked = jnp.take_along_axis(
        surface.reshape(shot_count, STEPS, -1),
        jnp.broadcast_to(flat_local[:, None, :], (shot_count, STEPS, record_count)),
        axis=2,
    )
    picked = jnp.where(holds[:, None, :], picked, jnp.float32(0.0))
    traces = lax.psum(picked, "slab")
    partial_image = jnp.zeros((layers, width_x, width_y), jnp.float32)
    corner = (jnp.int32(0), anchor_x[0], anchor_y[0])
    partial_image = lax.dynamic_update_slice(partial_image, energy_here[0], corner)
    summed = lax.psum_scatter(partial_image, "shot", scatter_dimension=1, tiled=True)
    return (traces, summed)


def small_vmem(name, **options):
    return dict(compiler_params=pltpu.CompilerParams(vmem_limit_bytes=VMEM_LIMIT, **options), name=name)


def strip_of(place, slabs):
    return place % 2 * (slabs // 2) + place // 2


def strip_pack(window_rows, window_cols, width_x, slabs, strip, records):
    tall = strip + 2 * STEPS

    def body(anchor_x, anchor_y, receivers, velocity, field, *rest):
        blocks, (facts, listed, speed, pressure, planes, sems) = rest[:slabs], rest[slabs:]
        mine = lax.axis_index("slab")
        top, left = anchor_x[0], anchor_y[0]
        begin = pl.multiple_of(jnp.minimum(top // SUBLANES * SUBLANES, width_x - window_rows - SUBLANES), SUBLANES)
        pltpu.make_async_copy(field.at[0, 0], pressure, sems.at[0]).start()
        for t in range(window_rows // SUBLANES + 1):
            place = window_rows if t == window_rows // SUBLANES else (begin + t * SUBLANES) % window_rows
            pltpu.make_async_copy(
                velocity.at[0, pl.ds(pl.multiple_of(begin + t * SUBLANES, SUBLANES), SUBLANES)],
                speed.at[pl.ds(pl.multiple_of(place, SUBLANES), SUBLANES)],
                sems.at[1],
            ).start()
        listing = pltpu.make_async_copy(receivers, listed, sems.at[2])
        listing.start()
        kinds = lax.broadcasted_iota(jnp.int32, facts.shape, 0)
        facts[...] = jnp.where(kinds == 0, top, left)
        pltpu.make_async_copy(field.at[0, 0], pressure, sems.at[0]).wait()
        rolled = pltpu.roll(pressure[...], left % window_cols, axis=1)
        rolled = pltpu.roll(rolled, (top + STEPS) % window_rows, axis=0)
        planes[0, :window_rows] = rolled
        planes[0, window_rows:] = rolled[: 2 * STEPS]
        pltpu.make_async_copy(velocity.at[0, : window_rows + SUBLANES], speed, sems.at[1]).wait()
        seam = pl.ds(pl.multiple_of(begin % window_rows, SUBLANES), SUBLANES)
        below = lax.broadcasted_iota(jnp.int32, (SUBLANES, 2 * window_cols), 0) < top - begin
        speed[seam] = jnp.where(below, speed[window_rows:], speed[seam])
        columns = lax.broadcasted_iota(jnp.int32, (window_rows, window_cols), 1)
        chosen = COURANT * jnp.where(
            columns >= left, speed[:window_rows, :window_cols], speed[:window_rows, window_cols:]
        )
        coefficient = pltpu.roll(chosen * chosen, STEPS, axis=0)
        planes[1, :window_rows] = coefficient
        planes[1, window_rows:] = coefficient[: 2 * STEPS]
        for k in range(slabs):
            start = pl.multiple_of(strip_of(mine ^ k, slabs) * strip, SUBLANES)
            blocks[k][:tall] = planes[0, pl.ds(start, tall), :]
            blocks[k][tall:] = planes[1, pl.ds(start, tall), :]
        listing.wait()

    hbm = pl.BlockSpec(memory_space=pltpu.HBM)
    smem = pl.BlockSpec(memory_space=pltpu.SMEM)
    vmem = pl.BlockSpec(memory_space=pltpu.VMEM)
    return pl.pallas_call(
        body,
        out_shape=[jax.ShapeDtypeStruct((2 * tall, window_cols), jnp.float32)] * slabs
        + [
            jax.ShapeDtypeStruct((SUBLANES, window_cols), jnp.int32),
            jax.ShapeDtypeStruct((1, records), jnp.int32),
        ],
        in_specs=[smem, smem] + [hbm] * 3,
        out_specs=[vmem] * (slabs + 2),
        scratch_shapes=[
            pltpu.VMEM((window_rows + SUBLANES, 2 * window_cols), jnp.float32),
            pltpu.VMEM((window_rows, window_cols), jnp.float32),
            pltpu.VMEM((2, window_rows + 2 * STEPS, window_cols), jnp.float32),
            pltpu.SemaphoreType.DMA((3,)),
        ],
        **small_vmem("strip_pack"),
    )


def strip_steps(window_rows, window_cols, slabs, strip, records, order, chunks):
    tall = strip + 2 * STEPS
    pieces = window_cols // LANES
    sizes = [len(chunk) * pieces * strip for chunk in chunks]
    heard_rows = records // LANES * STEPS

    def body(source, facts, receivers, *rest):
        blocks, outs = dict(zip(order, rest)), rest[slabs:-4]
        keeps, gives = outs[: len(chunks)], outs[len(chunks) :]
        fields, speeds, energy, surface = rest[-4:]
        mine = lax.axis_index("slab")
        core = lax.axis_index("shot") % 2
        top, left = facts[0:1], facts[1:2]
        for k in range(slabs):
            fields[0, mine ^ k] = blocks[k][:tall]
            speeds[mine ^ k] = blocks[k][tall:]
        rows = lax.broadcasted_iota(jnp.int32, (tall, window_cols), 0)
        columns = lax.broadcasted_iota(jnp.int32, (tall, window_cols), 1)
        begin = strip_of(mine, slabs) * strip - STEPS

        def local_row(row):
            return (row + top - begin + window_rows) % window_rows

        def local_column(column):
            return (column + left) % window_cols

        inside_up = jnp.where(rows != local_row(0), 1.0, 0.0)
        inside_down = jnp.where(rows != local_row(window_rows - 1), 1.0, 0.0)
        inside_left = jnp.where(columns != local_column(0), 1.0, 0.0)
        inside_right = jnp.where(columns != local_column(window_cols - 1), 1.0, 0.0)
        struck = (rows == local_row(source[0] // window_cols)) & (columns == local_column(source[0] % window_cols))
        source_term = jnp.where(struck, speeds[1], 0.0)
        for instant in range(STEPS):
            now, then = instant % 2, (instant + 1) % 2
            for level in range(slabs):
                current = fields[now, level]
                carried = 2.0 * current - fields[then, level] if instant else current
                laplacian = inside_up * pltpu.roll(current, 1, axis=0)
                laplacian = laplacian + inside_down * pltpu.roll(current, tall - 1, axis=0)
                laplacian = laplacian + inside_left * pltpu.roll(current, 1, axis=1)
                laplacian = laplacian + inside_right * pltpu.roll(current, window_cols - 1, axis=1)
                if level > 0:
                    laplacian = laplacian + fields[now, level - 1]
                if level < slabs - 1:
                    laplacian = laplacian + fields[now, level + 1]
                laplacian = laplacian - 6.0 * current
                advanced = carried + speeds[level] * laplacian
                if level == 1:
                    advanced = advanced + source_term * (AMPLITUDE * wavelet(instant))
                if level == 0:
                    surface[instant * tall : (instant + 1) * tall] = advanced
                if instant < STEPS - 1:
                    fields[then, level] = advanced
                square = advanced * advanced
                energy[level] = square if instant == 0 else energy[level] + square
        for parts, parity in ((gives, 1 - core), (keeps, core)):
            for out, chunk, size in zip(parts, chunks, sizes):
                for j, k in enumerate(chunk):
                    level = 2 * ((mine // 2) ^ k) + parity
                    for i in range(pieces):
                        at = (j * pieces + i) * strip
                        cells = energy[level, STEPS : STEPS + strip, i * LANES : (i + 1) * LANES]
                        out[at : at + strip] = cells / STEPS
                out[size : size + SUBLANES] = facts[:, :LANES].astype(jnp.float32)
        row = (receivers[...] // window_cols + top[:, :1]) % window_rows - begin
        column = (receivers[...] % window_cols + left[:, :1]) % window_cols
        row = jnp.where((row >= STEPS) & (row < STEPS + strip), row, -1)
        cells = lax.broadcasted_iota(jnp.int32, (window_cols, records), 0)
        chosen = jnp.where(cells == column, 1.0, 0.0)
        picked = jnp.dot(surface[...], chosen, precision=lax.Precision.HIGHEST, preferred_element_type=jnp.float32)
        places = lax.broadcasted_iota(jnp.int32, (tall, records), 0)
        for n in range(STEPS):
            own = jnp.where(places == row, picked[n * tall : (n + 1) * tall], 0.0)
            own = jnp.sum(own, axis=0, keepdims=True)
            for i in range(records // LANES):
                at = sizes[0] + SUBLANES + i * STEPS + n
                for out in (keeps[0], gives[0]):
                    out[at : at + 1] = own[:, i * LANES : (i + 1) * LANES]

    vmem = pl.BlockSpec(memory_space=pltpu.VMEM)
    return pl.pallas_call(
        body,
        out_shape=[
            jax.ShapeDtypeStruct((size + SUBLANES + (0 if c else heard_rows), LANES), jnp.float32)
            for c, size in enumerate(sizes)
        ]
        * 2,
        in_specs=[pl.BlockSpec(memory_space=pltpu.SMEM)] + [vmem] * (2 + slabs),
        out_specs=[vmem] * (2 * len(chunks)),
        scratch_shapes=[
            pltpu.VMEM((2, slabs, tall, window_cols), jnp.float32),
            pltpu.VMEM((slabs, tall, window_cols), jnp.float32),
            pltpu.VMEM((slabs, tall, window_cols), jnp.float32),
            pltpu.VMEM((STEPS * tall, window_cols), jnp.float32),
        ],
        **small_vmem("strip_steps"),
    )


def strip_share(window_rows, window_cols, width_y, rows_here, strip, records, count, tells):
    pieces = window_cols // LANES
    wide = width_y // LANES
    deep = count * pieces * strip
    heard_rows = records // LANES * STEPS

    def body(keep, got, *outs):
        mine, shot = lax.axis_index("slab"), lax.axis_index("shot")
        zone, side = mine // 2, mine % 2
        shares = (keep, got)
        tags = [share[deep : deep + SUBLANES].astype(jnp.int32) for share in shares]
        columns = lax.broadcasted_iota(jnp.int32, (strip, LANES), 1)
        for out, over_x in zip(outs, (1, 0)):
            to_shot = ((shot // 2) ^ over_x) * 2 + side
            rows = lax.broadcasted_iota(jnp.int32, (strip, LANES), 0) + to_shot * rows_here + zone * strip
            insides = []
            for tag in tags:
                down, along = rows - tag[0:1], columns - tag[1:2]
                tall = (down >= 0) & (down < window_rows)
                insides.append(
                    [tall & (along >= -i * LANES) & (along < window_cols - i * LANES) for i in range(wide)]
                )
            for j in range(count):
                for i in range(wide):
                    start = (j * pieces + i % pieces) * strip
                    parts = [
                        jnp.where(inside[i], share[start : start + strip], 0.0)
                        for share, inside in zip(shares, insides)
                    ]
                    at = (j * wide + i) * strip
                    out[at : at + strip] = parts[0] + parts[1]
        if tells:
            heard, told = outs[2:]
            same_core = shot % 2 == side
            heard[...] = jnp.where(same_core, keep[deep + SUBLANES :], got[deep + SUBLANES :])
            told[...] = jnp.where(same_core, got[deep + SUBLANES :], keep[deep + SUBLANES :])

    vmem = pl.BlockSpec(memory_space=pltpu.VMEM)
    sizes = [count * wide * strip] * 2 + [heard_rows] * (2 * tells)
    return pl.pallas_call(
        body,
        out_shape=[jax.ShapeDtypeStruct((size, LANES), jnp.float32) for size in sizes],
        in_specs=[vmem] * 2,
        out_specs=[vmem] * len(sizes),
        **small_vmem("strip_share"),
    )


def strip_sum(width_y, strip, records, count):
    deep = width_y // LANES * strip
    heard_rows = records // LANES * STEPS

    def body(come, own, heard_too, heard, *outs):
        for j, out in enumerate(outs):
            out[:deep] = own[j * deep : (j + 1) * deep] + come[j * deep : (j + 1) * deep]
            out[deep:] = heard[...] + heard_too[...]

    vmem = pl.BlockSpec(memory_space=pltpu.VMEM)
    return pl.pallas_call(
        body,
        out_shape=[jax.ShapeDtypeStruct((deep + heard_rows, LANES), jnp.float32)] * count,
        in_specs=[vmem] * 4,
        out_specs=[vmem] * count,
        **small_vmem("strip_sum"),
    )


def strip_place(width_y, rows_here, slabs, strip, records, order):
    wide = width_y // LANES
    pairs = slabs // 2

    def body(*rest):
        blocks, (traces, image) = dict(zip(order, rest)), rest[pairs:]
        zone = lax.axis_index("slab") // 2
        for k in range(pairs):
            start = pl.multiple_of((zone ^ k) * strip, SUBLANES)
            for i in range(wide):
                image[0, pl.ds(start, strip), i * LANES : (i + 1) * LANES] = blocks[k][i * strip : (i + 1) * strip]
        total = blocks[0][wide * strip :]
        for k in range(1, pairs):
            total = total + blocks[k][wide * strip :]
        for i in range(records // LANES):
            traces[0, :, i * LANES : (i + 1) * LANES] = total[i * STEPS : (i + 1) * STEPS]

    vmem = pl.BlockSpec(memory_space=pltpu.VMEM)
    return pl.pallas_call(
        body,
        out_shape=[
            jax.ShapeDtypeStruct((1, STEPS, records), jnp.float32),
            jax.ShapeDtypeStruct((1, rows_here, width_y), jnp.float32),
        ],
        in_specs=[vmem] * pairs,
        out_specs=[vmem] * 2,
        **small_vmem("strip_place"),
    )


def swap(array, axis, k):
    return lax.ppermute(array, axis, [(i, i ^ k) for i in range(lax.axis_size(axis))])


def far_first(count):
    half = count // 2
    return [*range(count - 1, half, -2), *range(count - 2, half - 1, -2), *range(half - 1, -1, -1)]


def cross(array, k):
    slabs, shots = lax.axis_size("slab"), lax.axis_size("shot")
    pairs = []
    for place in range(slabs):
        for shot in range(shots):
            side, core = place % 2, shot % 2
            to_place = ((place // 2) ^ k) * 2 + core
            to_shot = shot // 2 * 2 + side
            pairs.append((place * shots + shot, to_place * shots + to_shot))
    return lax.ppermute(array, ("slab", "shot"), pairs)


def by_strips(velocity, initial_field, anchor_x, anchor_y, source_cell, receivers):
    slabs, shots = lax.axis_size("slab"), lax.axis_size("shot")
    window_rows, window_cols = initial_field.shape[2:]
    width_y = velocity.shape[2]
    rows_here = velocity.shape[1] // shots
    strip = window_rows // slabs
    records = receivers.shape[1]
    velocity, initial_field, receivers = (
        pltpu.with_memory_space_constraint(array, pltpu.HBM) for array in (velocity, initial_field, receivers)
    )
    *packed, facts, listed = strip_pack(window_rows, window_cols, velocity.shape[1], slabs, strip, records)(
        anchor_x, anchor_y, receivers, velocity, initial_field
    )
    order = far_first(slabs)
    held = [swap(packed[k], "slab", k) if k else packed[k] for k in order]
    pairs = slabs // 2
    chunks = ((*range(pairs // 2, pairs),), (*range(pairs // 2 - 1, -1, -1),))
    zones = [k for chunk in chunks for k in chunk]
    outs = strip_steps(window_rows, window_cols, slabs, strip, records, order, chunks)(
        source_cell, facts, listed, *held
    )
    keeps, gives = outs[: len(chunks)], outs[len(chunks) :]
    gots = []
    for give in gives:
        gots.append(swap(give, "shot", 1))
    shares, notes = [], []
    for c, chunk in enumerate(chunks):
        leave, stay, *more = strip_share(
            window_rows, window_cols, width_y, rows_here, strip, records, len(chunk), c == 0
        )(keeps[c], gots[c])
        shares.append((swap(leave, "shot", 2), stay))
        notes += more
    heard, told = notes
    heard_too = swap(told, "slab", 1)
    back = []
    for chunk, (come, stay) in zip(chunks, shares):
        sums = strip_sum(width_y, strip, records, len(chunk))(come, stay, heard_too, heard)
        for part, k in zip(sums, chunk):
            back.append(cross(part, k))
    traces, image = strip_place(width_y, rows_here, slabs, strip, records, zones)(*back)
    return (traces, image)


def strips_fit(mesh, velocity, initial_field, receivers):
    slabs, shots = mesh.shape["slab"], mesh.shape["shot"]
    layers, width_x, width_y = velocity.shape
    shot_count, levels, window_rows, window_cols = initial_field.shape
    records = receivers.shape[1]
    return (
        layers == levels == slabs
        and slabs == 8
        and shot_count == shots == 4
        and width_x == 2 * window_rows
        and width_y == 2 * window_cols
        and window_rows % (slabs * SUBLANES) == 0
        and width_x // shots == window_rows // 2
        and window_rows // slabs + 2 * STEPS <= window_rows
        and window_cols % LANES == 0
        and records % (2 * LANES) == 0
        and (2 * STEPS) % SUBLANES == 0
    )


def solution(mesh):
    placed = (
        P("slab", None, None),
        P("shot", "slab", None, None),
        P("shot"),
        P("shot"),
        P("shot"),
        P("shot", None),
    )

    def whole(velocity, initial_field, anchor_x, anchor_y, source_cell, receivers):
        fit = strips_fit(mesh, velocity, initial_field, receivers)
        step = jax.shard_map(
            by_strips if fit else by_depth,
            mesh=mesh,
            in_specs=placed,
            out_specs=(P("shot", None, None), P("slab", "shot", None)),
            check_vma=False,
        )
        return step(velocity, initial_field, anchor_x, anchor_y, source_cell, receivers)

    return whole
```

```python
import math

import jax
import jax.numpy as jnp
from jax import lax
from jax.experimental import pallas as pl
from jax.experimental.pallas import tpu as pltpu
from jax.sharding import PartitionSpec as P


STEPS = 4


COURANT = 0.125
AMPLITUDE = 4.0

SUBLANES = 8
LANES = 128
VMEM_LIMIT = 16 * 1024 * 1024


def wavelet(instant):
    shifted = 0.8 * (instant - 1.5)
    return (1.0 - 2.0 * shifted * shifted) * math.exp(-shifted * shifted)


def with_halo(cells, sides, width):
    for axis, dim in sides:
        count = lax.axis_size(axis)
        ends = count - 1
        head = lax.slice_in_dim(cells, 0, width, axis=dim)
        tail = lax.slice_in_dim(cells, cells.shape[dim] - width, cells.shape[dim], axis=dim)
        cells = jnp.concatenate(
            [
                lax.ppermute(tail, axis, [(i, (i + 1) % count) for i in range(ends)]),
                cells,
                lax.ppermute(head, axis, [((i + 1) % count, i) for i in range(ends)]),
            ],
            axis=dim,
        )
    return cells


def propagate(speed, field, extend, source, depth_start):
    coefficient = jnp.square(COURANT * speed)
    column_count = speed.shape[3]
    depth_place = lax.broadcasted_iota(jnp.int32, speed.shape, 1) + depth_start
    row_place = lax.broadcasted_iota(jnp.int32, speed.shape, 2)
    column_place = lax.broadcasted_iota(jnp.int32, speed.shape, 3)
    source_row = (source // column_count)[:, None, None, None]
    source_column = (source % column_count)[:, None, None, None]
    struck = (depth_place == 1) & (row_place == source_row) & (column_place == source_column)
    source_term = jnp.where(struck, coefficient, jnp.float32(0.0))
    previous = field
    current = field
    energy = jnp.zeros(speed.shape, jnp.float32)
    surfaces = []
    for instant in range(STEPS):
        padded = extend(current)
        laplacian = padded[:, 2:, 1:-1, 1:-1] + padded[:, :-2, 1:-1, 1:-1]
        laplacian = laplacian + padded[:, 1:-1, 2:, 1:-1] + padded[:, 1:-1, :-2, 1:-1]
        laplacian = laplacian + padded[:, 1:-1, 1:-1, 2:] + padded[:, 1:-1, 1:-1, :-2]
        laplacian = laplacian - 6.0 * current
        advanced = 2.0 * current - previous + coefficient * laplacian
        advanced = advanced + source_term * (AMPLITUDE * wavelet(instant))
        energy = energy + advanced * advanced
        surfaces.append(advanced[:, 0])
        previous, current = (current, advanced)
    return (energy / STEPS, jnp.stack(surfaces, axis=1))


def by_depth(velocity, initial_field, anchor_x, anchor_y, source_cell, receivers):
    slab_index = lax.axis_index("slab")
    layers, width_x, width_y = velocity.shape
    shot_count = initial_field.shape[0]
    window_rows = initial_field.shape[2]
    window_cols = initial_field.shape[3]

    def cut_window(start_x, start_y):
        return lax.dynamic_slice(
            velocity, (jnp.int32(0), start_x, start_y), (layers, window_rows, window_cols)
        )

    windows = jax.vmap(cut_window)(anchor_x, anchor_y)
    depth_start = slab_index * layers

    def extend_depth(current):
        rimmed = with_halo(current, (("slab", 1),), 1)
        return jnp.pad(rimmed, ((0, 0), (0, 0), (1, 1), (1, 1)))

    energy_here, surface = propagate(windows, initial_field, extend_depth, source_cell, depth_start)
    local_rows = surface.shape[2]
    receiver_row = receivers // window_cols
    receiver_column = receivers % window_cols
    holds = (receiver_row >= 0) & (receiver_row < local_rows) & (depth_start == 0)
    flat_local = jnp.clip(receiver_row, 0, local_rows - 1) * window_cols + receiver_column
    record_count = receivers.shape[1]
    picked = jnp.take_along_axis(
        surface.reshape(shot_count, STEPS, -1),
        jnp.broadcast_to(flat_local[:, None, :], (shot_count, STEPS, record_count)),
        axis=2,
    )
    picked = jnp.where(holds[:, None, :], picked, jnp.float32(0.0))
    traces = lax.psum(picked, "slab")
    partial_image = jnp.zeros((layers, width_x, width_y), jnp.float32)
    corner = (jnp.int32(0), anchor_x[0], anchor_y[0])
    partial_image = lax.dynamic_update_slice(partial_image, energy_here[0], corner)
    summed = lax.psum_scatter(partial_image, "shot", scatter_dimension=1, tiled=True)
    return (traces, summed)


def small_vmem(name, **options):
    return dict(compiler_params=pltpu.CompilerParams(vmem_limit_bytes=VMEM_LIMIT, **options), name=name)


def strip_of(place, slabs):
    return place % 2 * (slabs // 2) + place // 2


def strip_pack(window_rows, window_cols, width_x, slabs, strip, records):
    tall = strip + 2 * STEPS

    def body(anchor_x, anchor_y, receivers, velocity, field, *rest):
        blocks, (facts, listed, speed, pressure, planes, sems) = rest[:slabs], rest[slabs:]
        mine = lax.axis_index("slab")
        top, left = anchor_x[0], anchor_y[0]
        begin = pl.multiple_of(jnp.minimum(top // SUBLANES * SUBLANES, width_x - window_rows - SUBLANES), SUBLANES)
        pltpu.make_async_copy(field.at[0, 0], pressure, sems.at[0]).start()
        for t in range(window_rows // SUBLANES + 1):
            place = window_rows if t == window_rows // SUBLANES else (begin + t * SUBLANES) % window_rows
            pltpu.make_async_copy(
                velocity.at[0, pl.ds(pl.multiple_of(begin + t * SUBLANES, SUBLANES), SUBLANES)],
                speed.at[pl.ds(pl.multiple_of(place, SUBLANES), SUBLANES)],
                sems.at[1],
            ).start()
        listing = pltpu.make_async_copy(receivers, listed, sems.at[2])
        listing.start()
        kinds = lax.broadcasted_iota(jnp.int32, facts.shape, 0)
        facts[...] = jnp.where(kinds == 0, top, left)
        pltpu.make_async_copy(field.at[0, 0], pressure, sems.at[0]).wait()
        rolled = pltpu.roll(pressure[...], left % window_cols, axis=1)
        rolled = pltpu.roll(rolled, (top + STEPS) % window_rows, axis=0)
        planes[0, :window_rows] = rolled
        planes[0, window_rows:] = rolled[: 2 * STEPS]
        pltpu.make_async_copy(velocity.at[0, : window_rows + SUBLANES], speed, sems.at[1]).wait()
        seam = pl.ds(pl.multiple_of(begin % window_rows, SUBLANES), SUBLANES)
        below = lax.broadcasted_iota(jnp.int32, (SUBLANES, 2 * window_cols), 0) < top - begin
        speed[seam] = jnp.where(below, speed[window_rows:], speed[seam])
        columns = lax.broadcasted_iota(jnp.int32, (window_rows, window_cols), 1)
        chosen = COURANT * jnp.where(
            columns >= left, speed[:window_rows, :window_cols], speed[:window_rows, window_cols:]
        )
        coefficient = pltpu.roll(chosen * chosen, STEPS, axis=0)
        planes[1, :window_rows] = coefficient
        planes[1, window_rows:] = coefficient[: 2 * STEPS]
        for k in range(slabs):
            start = pl.multiple_of(strip_of(mine ^ k, slabs) * strip, SUBLANES)
            blocks[k][:tall] = planes[0, pl.ds(start, tall), :]
            blocks[k][tall:] = planes[1, pl.ds(start, tall), :]
        listing.wait()

    hbm = pl.BlockSpec(memory_space=pltpu.HBM)
    smem = pl.BlockSpec(memory_space=pltpu.SMEM)
    vmem = pl.BlockSpec(memory_space=pltpu.VMEM)
    return pl.pallas_call(
        body,
        out_shape=[jax.ShapeDtypeStruct((2 * tall, window_cols), jnp.float32)] * slabs
        + [
            jax.ShapeDtypeStruct((SUBLANES, window_cols), jnp.int32),
            jax.ShapeDtypeStruct((1, records), jnp.int32),
        ],
        in_specs=[smem, smem] + [hbm] * 3,
        out_specs=[vmem] * (slabs + 2),
        scratch_shapes=[
            pltpu.VMEM((window_rows + SUBLANES, 2 * window_cols), jnp.float32),
            pltpu.VMEM((window_rows, window_cols), jnp.float32),
            pltpu.VMEM((2, window_rows + 2 * STEPS, window_cols), jnp.float32),
            pltpu.SemaphoreType.DMA((3,)),
        ],
        **small_vmem("strip_pack"),
    )


def strip_steps(window_rows, window_cols, slabs, strip, records, order, chunks):
    tall = strip + 2 * STEPS
    pieces = window_cols // LANES
    sizes = [len(chunk) * pieces * strip for chunk in chunks]
    heard_rows = records // LANES * STEPS

    def body(source, facts, receivers, *rest):
        blocks, outs = dict(zip(order, rest)), rest[slabs:-4]
        keeps, gives = outs[: len(chunks)], outs[len(chunks) :]
        fields, speeds, energy, surface = rest[-4:]
        mine = lax.axis_index("slab")
        core = lax.axis_index("shot") % 2
        top, left = facts[0:1], facts[1:2]
        for k in range(slabs):
            fields[0, mine ^ k] = blocks[k][:tall]
            speeds[mine ^ k] = blocks[k][tall:]
        rows = lax.broadcasted_iota(jnp.int32, (tall, window_cols), 0)
        columns = lax.broadcasted_iota(jnp.int32, (tall, window_cols), 1)
        begin = strip_of(mine, slabs) * strip - STEPS

        def local_row(row):
            return (row + top - begin + window_rows) % window_rows

        def local_column(column):
            return (column + left) % window_cols

        inside_up = jnp.where(rows != local_row(0), 1.0, 0.0)
        inside_down = jnp.where(rows != local_row(window_rows - 1), 1.0, 0.0)
        inside_left = jnp.where(columns != local_column(0), 1.0, 0.0)
        inside_right = jnp.where(columns != local_column(window_cols - 1), 1.0, 0.0)
        struck = (rows == local_row(source[0] // window_cols)) & (columns == local_column(source[0] % window_cols))
        source_term = jnp.where(struck, speeds[1], 0.0)
        for instant in range(STEPS):
            now, then = instant % 2, (instant + 1) % 2
            for level in range(slabs):
                current = fields[now, level]
                carried = 2.0 * current - fields[then, level] if instant else current
                laplacian = inside_up * pltpu.roll(current, 1, axis=0)
                laplacian = laplacian + inside_down * pltpu.roll(current, tall - 1, axis=0)
                laplacian = laplacian + inside_left * pltpu.roll(current, 1, axis=1)
                laplacian = laplacian + inside_right * pltpu.roll(current, window_cols - 1, axis=1)
                if level > 0:
                    laplacian = laplacian + fields[now, level - 1]
                if level < slabs - 1:
                    laplacian = laplacian + fields[now, level + 1]
                laplacian = laplacian - 6.0 * current
                advanced = carried + speeds[level] * laplacian
                if level == 1:
                    advanced = advanced + source_term * (AMPLITUDE * wavelet(instant))
                if level == 0:
                    surface[instant * tall : (instant + 1) * tall] = advanced
                if instant < STEPS - 1:
                    fields[then, level] = advanced
                square = advanced * advanced
                energy[level] = square if instant == 0 else energy[level] + square
        for parts, parity in ((gives, 1 - core), (keeps, core)):
            for out, chunk, size in zip(parts, chunks, sizes):
                for j, k in enumerate(chunk):
                    level = 2 * ((mine // 2) ^ k) + parity
                    for i in range(pieces):
                        at = (j * pieces + i) * strip
                        cells = energy[level, STEPS : STEPS + strip, i * LANES : (i + 1) * LANES]
                        out[at : at + strip] = cells / STEPS
                out[size : size + SUBLANES] = facts[:, :LANES].astype(jnp.float32)
        row = (receivers[...] // window_cols + top[:, :1]) % window_rows - begin
        column = (receivers[...] % window_cols + left[:, :1]) % window_cols
        row = jnp.where((row >= STEPS) & (row < STEPS + strip), row, -1)
        cells = lax.broadcasted_iota(jnp.int32, (window_cols, records), 0)
        chosen = jnp.where(cells == column, 1.0, 0.0)
        picked = jnp.dot(surface[...], chosen, precision=lax.Precision.HIGHEST, preferred_element_type=jnp.float32)
        places = lax.broadcasted_iota(jnp.int32, (tall, records), 0)
        for n in range(STEPS):
            own = jnp.where(places == row, picked[n * tall : (n + 1) * tall], 0.0)
            own = jnp.sum(own, axis=0, keepdims=True)
            for i in range(records // LANES):
                at = sizes[0] + SUBLANES + i * STEPS + n
                for out in (keeps[0], gives[0]):
                    out[at : at + 1] = own[:, i * LANES : (i + 1) * LANES]

    vmem = pl.BlockSpec(memory_space=pltpu.VMEM)
    return pl.pallas_call(
        body,
        out_shape=[
            jax.ShapeDtypeStruct((size + SUBLANES + (0 if c else heard_rows), LANES), jnp.float32)
            for c, size in enumerate(sizes)
        ]
        * 2,
        in_specs=[pl.BlockSpec(memory_space=pltpu.SMEM)] + [vmem] * (2 + slabs),
        out_specs=[vmem] * (2 * len(chunks)),
        scratch_shapes=[
            pltpu.VMEM((2, slabs, tall, window_cols), jnp.float32),
            pltpu.VMEM((slabs, tall, window_cols), jnp.float32),
            pltpu.VMEM((slabs, tall, window_cols), jnp.float32),
            pltpu.VMEM((STEPS * tall, window_cols), jnp.float32),
        ],
        **small_vmem("strip_steps"),
    )


def strip_share(window_rows, window_cols, width_y, rows_here, strip, records, count, tells):
    pieces = window_cols // LANES
    wide = width_y // LANES
    deep = count * pieces * strip
    heard_rows = records // LANES * STEPS

    def body(keep, got, *outs):
        mine, shot = lax.axis_index("slab"), lax.axis_index("shot")
        zone, side = mine // 2, mine % 2
        shares = (keep, got)
        tags = [share[deep : deep + SUBLANES].astype(jnp.int32) for share in shares]
        columns = lax.broadcasted_iota(jnp.int32, (strip, LANES), 1)
        for out, over_x in zip(outs, (1, 0)):
            to_shot = ((shot // 2) ^ over_x) * 2 + side
            rows = lax.broadcasted_iota(jnp.int32, (strip, LANES), 0) + to_shot * rows_here + zone * strip
            insides = []
            for tag in tags:
                down, along = rows - tag[0:1], columns - tag[1:2]
                tall = (down >= 0) & (down < window_rows)
                insides.append(
                    [tall & (along >= -i * LANES) & (along < window_cols - i * LANES) for i in range(wide)]
                )
            for j in range(count):
                for i in range(wide):
                    start = (j * pieces + i % pieces) * strip
                    parts = [
                        jnp.where(inside[i], share[start : start + strip], 0.0)
                        for share, inside in zip(shares, insides)
                    ]
                    at = (j * wide + i) * strip
                    out[at : at + strip] = parts[0] + parts[1]
        if tells:
            heard, told = outs[2:]
            same_core = shot % 2 == side
            heard[...] = jnp.where(same_core, keep[deep + SUBLANES :], got[deep + SUBLANES :])
            told[...] = jnp.where(same_core, got[deep + SUBLANES :], keep[deep + SUBLANES :])

    vmem = pl.BlockSpec(memory_space=pltpu.VMEM)
    sizes = [count * wide * strip] * 2 + [heard_rows] * (2 * tells)
    return pl.pallas_call(
        body,
        out_shape=[jax.ShapeDtypeStruct((size, LANES), jnp.float32) for size in sizes],
        in_specs=[vmem] * 2,
        out_specs=[vmem] * len(sizes),
        **small_vmem("strip_share"),
    )


def strip_sum(width_y, strip, records, count):
    deep = width_y // LANES * strip
    heard_rows = records // LANES * STEPS

    def body(come, own, heard_too, heard, *outs):
        for j, out in enumerate(outs):
            out[:deep] = own[j * deep : (j + 1) * deep] + come[j * deep : (j + 1) * deep]
            out[deep:] = heard[...] + heard_too[...]

    vmem = pl.BlockSpec(memory_space=pltpu.VMEM)
    return pl.pallas_call(
        body,
        out_shape=[jax.ShapeDtypeStruct((deep + heard_rows, LANES), jnp.float32)] * count,
        in_specs=[vmem] * 4,
        out_specs=[vmem] * count,
        **small_vmem("strip_sum"),
    )


def strip_place(width_y, rows_here, slabs, strip, records, order):
    wide = width_y // LANES
    pairs = slabs // 2

    def body(*rest):
        blocks, (traces, image) = dict(zip(order, rest)), rest[pairs:]
        zone = lax.axis_index("slab") // 2
        for k in range(pairs):
            start = pl.multiple_of((zone ^ k) * strip, SUBLANES)
            for i in range(wide):
                image[0, pl.ds(start, strip), i * LANES : (i + 1) * LANES] = blocks[k][i * strip : (i + 1) * strip]
        total = blocks[0][wide * strip :]
        for k in range(1, pairs):
            total = total + blocks[k][wide * strip :]
        for i in range(records // LANES):
            traces[0, :, i * LANES : (i + 1) * LANES] = total[i * STEPS : (i + 1) * STEPS]

    vmem = pl.BlockSpec(memory_space=pltpu.VMEM)
    return pl.pallas_call(
        body,
        out_shape=[
            jax.ShapeDtypeStruct((1, STEPS, records), jnp.float32),
            jax.ShapeDtypeStruct((1, rows_here, width_y), jnp.float32),
        ],
        in_specs=[vmem] * pairs,
        out_specs=[vmem] * 2,
        **small_vmem("strip_place"),
    )


def swap(array, axis, k):
    return lax.ppermute(array, axis, [(i, i ^ k) for i in range(lax.axis_size(axis))])


def far_first():
    return [7, 5, 6, 4, 1, 3, 2, 0]


def cross(array, k):
    slabs, shots = lax.axis_size("slab"), lax.axis_size("shot")
    pairs = []
    for place in range(slabs):
        for shot in range(shots):
            side, core = place % 2, shot % 2
            to_place = ((place // 2) ^ k) * 2 + core
            to_shot = shot // 2 * 2 + side
            pairs.append((place * shots + shot, to_place * shots + to_shot))
    return lax.ppermute(array, ("slab", "shot"), pairs)


def by_strips(velocity, initial_field, anchor_x, anchor_y, source_cell, receivers):
    slabs, shots = lax.axis_size("slab"), lax.axis_size("shot")
    window_rows, window_cols = initial_field.shape[2:]
    width_y = velocity.shape[2]
    rows_here = velocity.shape[1] // shots
    strip = window_rows // slabs
    records = receivers.shape[1]
    velocity, initial_field, receivers = (
        pltpu.with_memory_space_constraint(array, pltpu.HBM) for array in (velocity, initial_field, receivers)
    )
    *packed, facts, listed = strip_pack(window_rows, window_cols, velocity.shape[1], slabs, strip, records)(
        anchor_x, anchor_y, receivers, velocity, initial_field
    )
    order = far_first()
    held = [swap(packed[k], "slab", k) if k else packed[k] for k in order]
    pairs = slabs // 2
    chunks = ((*range(pairs // 2, pairs),), (*range(pairs // 2 - 1, -1, -1),))
    zones = [k for chunk in chunks for k in chunk]
    outs = strip_steps(window_rows, window_cols, slabs, strip, records, order, chunks)(
        source_cell, facts, listed, *held
    )
    keeps, gives = outs[: len(chunks)], outs[len(chunks) :]
    gots = []
    for give in gives:
        gots.append(swap(give, "shot", 1))
    shares, notes = [], []
    for c, chunk in enumerate(chunks):
        leave, stay, *more = strip_share(
            window_rows, window_cols, width_y, rows_here, strip, records, len(chunk), c == 0
        )(keeps[c], gots[c])
        shares.append((swap(leave, "shot", 2), stay))
        notes += more
    heard, told = notes
    heard_too = swap(told, "slab", 1)
    back = []
    for chunk, (come, stay) in zip(chunks, shares):
        sums = strip_sum(width_y, strip, records, len(chunk))(come, stay, heard_too, heard)
        for part, k in zip(sums, chunk):
            back.append(cross(part, k))
    traces, image = strip_place(width_y, rows_here, slabs, strip, records, zones)(*back)
    return (traces, image)


def strips_fit(mesh, velocity, initial_field, receivers):
    slabs, shots = mesh.shape["slab"], mesh.shape["shot"]
    layers, width_x, width_y = velocity.shape
    shot_count, levels, window_rows, window_cols = initial_field.shape
    records = receivers.shape[1]
    return (
        layers == levels == slabs
        and slabs == 8
        and shot_count == shots == 4
        and width_x == 2 * window_rows
        and width_y == 2 * window_cols
        and window_rows % (slabs * SUBLANES) == 0
        and width_x // shots == window_rows // 2
        and window_rows // slabs + 2 * STEPS <= window_rows
        and window_cols % LANES == 0
        and records % (2 * LANES) == 0
        and (2 * STEPS) % SUBLANES == 0
    )


def solution(mesh):
    placed = (
        P("slab", None, None),
        P("shot", "slab", None, None),
        P("shot"),
        P("shot"),
        P("shot"),
        P("shot", None),
    )

    def whole(velocity, initial_field, anchor_x, anchor_y, source_cell, receivers):
        fit = strips_fit(mesh, velocity, initial_field, receivers)
        step = jax.shard_map(
            by_strips if fit else by_depth,
            mesh=mesh,
            in_specs=placed,
            out_specs=(P("shot", None, None), P("slab", "shot", None)),
            check_vma=False,
        )
        return step(velocity, initial_field, anchor_x, anchor_y, source_cell, receivers)

    return whole
```
